256 devices in a mesh: gx: 16 (over y, z_lo, core), yz: 16 (over x, z_hi).
Axes of the slice: x: 4, y: 4, z: 8 (z_hi: 4, z_lo: 2; z = z_hi * 2 + z_lo), core: 2. Of those that a mesh axis runs over, the one named last changes fastest.
Arguments:
- fluid_offsets: float32 [3, 16, 48, 64, 128], P(None, None, 'gx', 'yz'), may hold values from 0 to 1
- fluid_velocity: float32 [3, 16, 48, 64, 128], P(None, None, 'gx', 'yz'), may hold values from -6 to 6
- fluid_density: float32 [16, 48, 64, 128], P(None, 'gx', 'yz'), may hold values from 0.97 to 1.03
- fluid_counts: int32 [48, 64, 128], P('gx', 'yz'), may hold values from 0 to 16, as said below
- wall_offsets: float32 [3, 4, 48, 64, 128], P(None, None, 'gx', 'yz'), may hold values from 0 to 1
- wall_counts: int32 [48, 64, 128], P('gx', 'yz'), may hold values from 0 to 4, as said below
Outputs:
- velocity_step: float32 [3, 16, 48, 64, 128], P(None, None, 'gx', 'yz')
- density_rate: float32 [16, 48, 64, 128], P(None, 'gx', 'yz')
The draws below stay inside these ranges and needn't reach their ends.
Inputs may be any that keep to these rules, and one draw needn't show every extreme that they name: `fluid_counts`: slots 0 to count - 1 of a cell hold fluid particles; cells inside solid obstacles hold none. `wall_counts`: slots 0 to count - 1 of a cell hold wall particles; every cell of the bottom layer (last index 0) holds 4.
All inputs are finite; a program needn't handle non-finite values.
Results may differ from the reference program's by a relative error of at most 0.0003.
Values sent between devices are 32-bit elements; how exact they have to be, the bound alone decides.
No kernel may reach another device: no remote copies, remote signals or barrier semaphores. Data moves between devices by JAX's collectives and lax.ppermute only.
A program may use at most 128 MiB of HBM per device.

```python
import jax
import jax.numpy as jnp
from jax import lax

SLOTS = 16
WALL_SLOTS = 4
CX = 3
CZ = 128
NX = 48
NY = 64


def obstacle_cells(key):
    box_x = max(2, NX // 12)
    box_y = max(2, NY // 12)
    box_z = max(2, CZ // 16)
    base = jax.random.fold_in(key, 29)
    corner_x = jax.random.randint(jax.random.fold_in(base, 1), (3,), NX // 4, NX - box_x, dtype=jnp.int32)
    corner_y = jax.random.randint(jax.random.fold_in(base, 2), (3,), 1, NY - 1 - box_y, dtype=jnp.int32)
    cell_x = jnp.arange(NX, dtype=jnp.int32)[None, :, None, None]
    cell_y = jnp.arange(NY, dtype=jnp.int32)[None, None, :, None]
    cell_z = jnp.arange(CZ, dtype=jnp.int32)[None, None, None, :]
    low_x = corner_x[:, None, None, None]
    low_y = corner_y[:, None, None, None]
    inside = (cell_x >= low_x) & (cell_x < low_x + box_x) & (cell_y >= low_y) & (cell_y < low_y + box_y) & (cell_z < box_z)
    return jnp.any(inside, axis=0)


def draw_fluid_counts(key, part):
    column = jnp.arange(NX, dtype=jnp.int32)[:, None, None]
    limit = jnp.maximum(1, SLOTS * (NX + 7 * column + 7) // (8 * NX))
    limit = jnp.broadcast_to(limit, (NX, NY, CZ)).astype(jnp.int32)
    counts = jax.random.randint(key, (NX, NY, CZ), 1, limit + 1, dtype=jnp.int32)
    counts = counts.at[NX - 1, :, 0].set(SLOTS)
    counts = jnp.where(obstacle_cells(key), 0, counts)
    return counts.astype(jnp.int32)


def draw_wall_counts(key, part):
    cell_x = jnp.arange(NX, dtype=jnp.int32)[:, None, None]
    cell_y = jnp.arange(NY, dtype=jnp.int32)[None, :, None]
    cell_z = jnp.arange(CZ, dtype=jnp.int32)[None, None, :]
    solid = (cell_z == 0) | (cell_y == 0) | (cell_y == NY - 1) | (cell_x == 0)
    solid = solid | obstacle_cells(key)
    counts = jnp.where(solid, WALL_SLOTS, 0)
    return counts.astype(jnp.int32)


def levels(key, shape, split, least, high):
    def one(position, shards_of):
        steps = jax.random.uniform(jax.random.fold_in(jax.random.fold_in(key, 6), position), (shards_of,), jnp.float32, least / len(split), high / len(split))
        return jnp.repeat(jnp.exp(steps), shape[position] // shards_of).reshape((-1,) + (1,) * (len(shape) - position - 1))

    factor_of = one(*split[0])
    for cut in split[1:]:
        factor_of = factor_of * one(*cut)
    return factor_of


def bell_draw(stream_key, shape, scale, bound, split=(), kind=jnp.bfloat16):
    array = scale * jax.random.normal(stream_key, shape, jnp.float32)
    if split:
        array = array * levels(stream_key, shape, split, -0.22, 0.18)
    return jnp.clip(array, -bound, bound).astype(kind)


def setup_inputs(seed: int = 0) -> dict:
    key_list = jax.random.split(jax.random.key(seed), 7)
    fluid_offsets = jnp.clip(1.0 * jax.random.uniform(key_list[0], (3, SLOTS, NX, NY, CZ), jnp.float32) ** levels(key_list[0], (3, SLOTS, NX, NY, CZ), ((2, 16), (3, 16)), -0.2, 0.2), 0.0, 1.0)
    fluid_velocity = bell_draw(key_list[1], (3, SLOTS, NX, NY, CZ), 1.0, 6.0, ((2, 16), (3, 16)), jnp.float32)
    fluid_density = jnp.clip(0.97 + 0.059999943 * jax.random.uniform(key_list[2], (SLOTS, NX, NY, CZ), jnp.float32) ** levels(key_list[2], (SLOTS, NX, NY, CZ), ((1, 16), (2, 16)), -0.2, 0.2), 0.97, 1.03)
    fluid_counts = draw_fluid_counts(jax.random.fold_in(key_list[6], 71), 0)
    wall_offsets = jnp.clip(1.0 * jax.random.uniform(key_list[4], (3, WALL_SLOTS, NX, NY, CZ), jnp.float32) ** levels(key_list[4], (3, WALL_SLOTS, NX, NY, CZ), ((2, 16), (3, 16)), -0.2, 0.2), 0.0, 1.0)
    wall_counts = draw_wall_counts(jax.random.fold_in(key_list[6], 71), 0)
    return dict(fluid_offsets=fluid_offsets, fluid_velocity=fluid_velocity, fluid_density=fluid_density, fluid_counts=fluid_counts, wall_offsets=wall_offsets, wall_counts=wall_counts)


gravity = 2.0
particle_mass = 0.125
smoothing = 0.5
sound_speed = 10.0
viscosity_alpha = 0.2
stiffness = 100.0 / 7.0
shepard_floor = 0.125
courant = 0.25
epsilon = 1e-06

def kernel(vector_x, vector_y, vector_z):
    squared = vector_x * vector_x + vector_y * vector_y + vector_z * vector_z
    distance = jnp.sqrt(squared)
    remain = jnp.maximum(1.0 - distance, 0.0)
    remain_cube = remain * remain * remain
    return (squared, remain_cube * remain * (4.0 * distance + 1.0), 20.0 * remain_cube)

def pack_fluid(offsets, velocity, density, counts):
    slot_level = lax.broadcasted_iota(jnp.int32, (offsets.shape[1],) + counts.shape, 0)
    masses = jnp.where(slot_level < counts[None], particle_mass, 0.0).astype(offsets.dtype)
    pressure = stiffness * (density ** 7 - 1.0)
    pressure_term = pressure / (density * density)
    return jnp.concatenate([offsets, velocity, density[None], pressure[None], pressure_term[None], masses[None]], 0)

def pack_walls(offsets, counts):
    slot_level = lax.broadcasted_iota(jnp.int32, (offsets.shape[1],) + counts.shape, 0)
    masses = jnp.where(slot_level < counts[None], particle_mass, 0.0).astype(offsets.dtype)
    return jnp.concatenate([offsets, masses[None]], 0)

def extrapolate(wall_geom, fluid_pad):
    extent = wall_geom.shape[2:]
    kernel_sum = jnp.zeros(wall_geom.shape[1:], wall_geom.dtype)
    weighted = jnp.zeros(wall_geom.shape[1:], wall_geom.dtype)
    for move_x in (-1, 0, 1):
        for move_y in (-1, 0, 1):
            for move_z in (-1, 0, 1):
                source = fluid_pad[:, :, 1 + move_x:1 + move_x + extent[0], 1 + move_y:1 + move_y + extent[1], 1 + move_z:1 + move_z + extent[2]]
                vector_x = wall_geom[0][:, None] - source[0][None] - move_x
                vector_y = wall_geom[1][:, None] - source[1][None] - move_y
                vector_z = wall_geom[2][:, None] - source[2][None] - move_z
                squared, weight, slope = kernel(vector_x, vector_y, vector_z)
                massed = source[9][None] * weight
                kernel_sum = kernel_sum + lax.optimization_barrier(jnp.sum(massed, axis=1))
                weighted = weighted + lax.optimization_barrier(jnp.sum(massed * (source[7][None] - gravity * source[6][None] * vector_z), axis=1))
    return weighted / jnp.maximum(kernel_sum, shepard_floor)

def interact(targets, fluid_pad, wall_pad):
    extent = targets.shape[2:]
    shape_one = targets.shape[1:]
    force_x = jnp.zeros(shape_one, targets.dtype)
    force_y = jnp.zeros(shape_one, targets.dtype)
    force_z = jnp.zeros(shape_one, targets.dtype)
    density_rate = jnp.zeros(shape_one, targets.dtype)
    damping = viscosity_alpha * sound_speed * smoothing
    for move_x in (-1, 0, 1):
        for move_y in (-1, 0, 1):
            for move_z in (-1, 0, 1):
                window = (slice(None), slice(None), slice(1 + move_x, 1 + move_x + extent[0]), slice(1 + move_y, 1 + move_y + extent[1]), slice(1 + move_z, 1 + move_z + extent[2]))
                source = fluid_pad[window]
                near_wall = wall_pad[window]
                vector_x = targets[0][:, None] - source[0][None] - move_x
                vector_y = targets[1][:, None] - source[1][None] - move_y
                vector_z = targets[2][:, None] - source[2][None] - move_z
                squared, weight, slope = kernel(vector_x, vector_y, vector_z)
                approach = (targets[3][:, None] - source[3][None]) * vector_x + (targets[4][:, None] - source[4][None]) * vector_y + (targets[5][:, None] - source[5][None]) * vector_z
                mean_density = 0.5 * (targets[6][:, None] + source[6][None])
                viscous = -damping * jnp.minimum(approach, 0.0) / ((squared + 0.01 * smoothing * smoothing) * mean_density)
                massed = source[9][None] * slope
                factor = massed * (targets[8][:, None] + source[8][None] + viscous)
                force_x = force_x + lax.optimization_barrier(jnp.sum(factor * vector_x, axis=1))
                force_y = force_y + lax.optimization_barrier(jnp.sum(factor * vector_y, axis=1))
                force_z = force_z + lax.optimization_barrier(jnp.sum(factor * vector_z, axis=1))
                density_rate = density_rate - lax.optimization_barrier(jnp.sum(massed * approach, axis=1))
                vector_x = targets[0][:, None] - near_wall[0][None] - move_x
                vector_y = targets[1][:, None] - near_wall[1][None] - move_y
                vector_z = targets[2][:, None] - near_wall[2][None] - move_z
                squared, weight, slope = kernel(vector_x, vector_y, vector_z)
                approach = targets[3][:, None] * vector_x + targets[4][:, None] * vector_y + targets[5][:, None] * vector_z
                mean_density = 0.5 * (targets[6][:, None] + 1.0)
                viscous = -damping * jnp.minimum(approach, 0.0) / ((squared + 0.01 * smoothing * smoothing) * mean_density)
                massed = near_wall[4][None] * slope
                factor = massed * (targets[8][:, None] + near_wall[3][None] + viscous)
                force_x = force_x + lax.optimization_barrier(jnp.sum(factor * vector_x, axis=1))
                force_y = force_y + lax.optimization_barrier(jnp.sum(factor * vector_y, axis=1))
                force_z = force_z + lax.optimization_barrier(jnp.sum(factor * vector_z, axis=1))
                density_rate = density_rate - lax.optimization_barrier(jnp.sum(massed * approach, axis=1))
    return (jnp.stack([force_x, force_y, force_z - gravity]), density_rate)

def pad_all(values):
    return jnp.pad(values, ((0, 0), (0, 0), (1, 1), (1, 1), (1, 1)))

def reference(fluid_offsets, fluid_velocity, fluid_density, fluid_counts, wall_offsets, wall_counts):
    fluid_data = pack_fluid(fluid_offsets, fluid_velocity, fluid_density, fluid_counts)
    wall_geom = pack_walls(wall_offsets, wall_counts)
    fluid_pad = pad_all(fluid_data)
    blocks = NX // CX

    def pressure_block(index):
        first_row = (index * CX).astype(jnp.int32)
        geometry = lax.dynamic_slice_in_dim(wall_geom, first_row, CX, 2)
        nearby = lax.dynamic_slice_in_dim(fluid_pad, first_row, CX + 2, 2)
        return extrapolate(geometry, nearby)
    indices = jnp.arange(blocks, dtype=jnp.int32)
    pressures = lax.map(pressure_block, indices)
    pressures = jnp.moveaxis(pressures, 0, 1).reshape((WALL_SLOTS, NX, NY, CZ))
    wall_data = jnp.concatenate([wall_geom[:3], pressures[None], wall_geom[3:]], 0)
    wall_pad = pad_all(wall_data)

    def force_block(index):
        first_row = (index * CX).astype(jnp.int32)
        targets = lax.dynamic_slice_in_dim(fluid_data, first_row, CX, 2)
        nearby = lax.dynamic_slice_in_dim(fluid_pad, first_row, CX + 2, 2)
        near_walls = lax.dynamic_slice_in_dim(wall_pad, first_row, CX + 2, 2)
        return interact(targets, nearby, near_walls)
    forces, rates = lax.map(force_block, indices)
    forces = jnp.moveaxis(forces, 0, 2).reshape((3, SLOTS, NX, NY, CZ))
    rates = jnp.moveaxis(rates, 0, 1).reshape((SLOTS, NX, NY, CZ))
    occupied = (fluid_data[9] > 0.0).astype(fluid_data.dtype)
    acceleration = forces * occupied[None]
    density_rate = rates * occupied
    largest = jnp.max(lax.optimization_barrier(jnp.sum(acceleration * acceleration, axis=0)))
    time_step = courant * jnp.sqrt(smoothing / (jnp.sqrt(largest) + epsilon))
    return (time_step * acceleration, density_rate)
```

```python
from functools import partial

import jax
import jax.numpy as jnp
import numpy as np
from jax import lax
from jax.experimental import pallas as pl
from jax.experimental.pallas import tpu as pltpu
from jax.sharding import Mesh
from jax.sharding import PartitionSpec as P

GX = ("gx_0", "gx_1", "gx_2")
YZ = ("yz_0", "yz_1")

GRAVITY = 2.0
STIFFNESS = 100.0 / 7.0
SOFT = 0.0025
SCALE = 2.5
FAR = 1.0e6
PAD = -1.0e6
BX, BY, SLOTS, WALLS = 3, 4, 16, 4
COLS = BX * BY
ROWS = 144
WIRE = 128
NEAR = 64
WALL = 112
PART = (0, 16, 32, 48, 128, 64, 80, 96)
F32 = jnp.float32


def rows8(ref, base):
    return ref[pl.ds(pl.multiple_of(base, 8), 8), :]


def spread(ref, row):
    return ref[pl.ds(row, 8, stride=0), :]


def put8(ref, base, value):
    ref[pl.ds(pl.multiple_of(base, 8), 8), :] = value


def lanes():
    return lax.broadcasted_iota(jnp.int32, (8, 128), 1)


def shifted(value, move, fill=None):
    out = pltpu.roll(value, (-move) % 128, 1)
    if fill is None:
        return out
    return jnp.where(lanes() == (127 if move > 0 else 0), fill, out)


def slope(dx, dy, dz):
    squared = dx * dx + dy * dy + dz * dz
    distance = squared * lax.rsqrt(jnp.maximum(squared, 1e-30))
    remain = jnp.maximum(1.0 - distance, 0.0)
    return squared, remain * remain * remain


def weight(dx, dy, dz):
    squared = dx * dx + dy * dy + dz * dz
    distance = squared * lax.rsqrt(jnp.maximum(squared, 1e-30))
    remain = jnp.maximum(1.0 - distance, 0.0)
    twice = remain * remain
    return (twice * twice) * (4.0 * distance + 1.0)


def fluid_pair(t, s):
    dx, dy, dz = t[0] - s[0], t[1] - s[1], t[2] - s[2]
    squared, cube = slope(dx, dy, dz)
    approach = (t[5] - s[5]) * dx + (t[6] - s[6]) * dy + (t[7] - s[7]) * dz
    below = (squared + SOFT) * (t[3] + s[3])
    viscous = jnp.minimum(approach, 0.0) * pl.reciprocal(below, approx=True)
    factor = cube * ((t[4] + s[4]) - viscous)
    return factor * dx, factor * dy, factor * dz, cube * approach


def wall_pair(t, s):
    dx, dy, dz = t[0] - s[0], t[1] - s[1], t[2] - s[2]
    squared, cube = slope(dx, dy, dz)
    approach = t[5] * dx + t[6] * dy + t[7] * dz
    below = (squared + SOFT) * t[3]
    viscous = jnp.minimum(approach, 0.0) * pl.reciprocal(below, approx=True)
    factor = cube * ((t[4] + s[3]) - viscous)
    return factor * dx, factor * dy, factor * dz, cube * approach


def pressure_term(rho):
    rho2 = rho * rho
    return (STIFFNESS * ((rho2 * rho2) * (rho2 * rho) - 1.0)) / rho2


def pack_body(
    off_in, vel_in, den_in, cnt_in, woff_in, wcnt_in, own, right, left, up, down,
    off, vel, den, cnt, woff, wcnt, sems,
):
    copies = [
        pltpu.make_async_copy(src, dst, sems.at[n])
        for n, (src, dst) in enumerate(
            zip((off_in, vel_in, den_in, cnt_in, woff_in, wcnt_in), (off, vel, den, cnt, woff, wcnt))
        )
    ]
    for copy in copies:
        copy.start()
    for copy in copies:
        copy.wait()
    slot = lax.broadcasted_iota(jnp.int32, (SLOTS, 128), 0)
    wslot = lax.broadcasted_iota(jnp.int32, (WALLS, 128), 0)
    for q in range(COLS):
        x, y = divmod(q, BY)
        base = q * ROWS
        live = slot < jnp.broadcast_to(cnt[x, y : y + 1, :], (SLOTS, 128))

        def take(ref, part):
            return ref[pl.ds(part * SLOTS * COLS + q, SLOTS, stride=COLS), :]

        rho = take(den, 0)
        parts = (
            jnp.where(live, take(off, 0) + float(x), FAR),
            take(off, 1) + float(y),
            take(off, 2),
            0.5 * rho,
            pressure_term(rho),
            take(vel, 0),
            take(vel, 1),
            take(vel, 2),
        )
        for at, part in zip(PART, parts):
            own[base + at : base + at + 16, :] = part
        live = wslot < jnp.broadcast_to(wcnt[x, y : y + 1, :], (WALLS, 128))

        def wtake(part):
            return woff[pl.ds(part * WALLS * COLS + q, WALLS, stride=COLS), :]

        base += WALL
        own[base : base + 4, :] = jnp.where(live, wtake(0) + float(x), FAR)
        own[base + 4 : base + 8, :] = wtake(1) + float(y)
        own[base + 8 : base + 12, :] = wtake(2)
        own[base + 12 : base + 16, :] = jnp.where(live, 1.0, 0.0)
    for ref, first in ((right, BX - 1), (left, 0)):
        for y in range(BY):
            base = (first * BY + y) * ROWS
            ref[y * WIRE : (y + 1) * WIRE, :] = own[base : base + WIRE, :]
            base = (1 * BY + y) * ROWS
            start = BY * WIRE + y * NEAR
            ref[start : start + NEAR, :] = own[base : base + NEAR, :]
    for ref, near, next_ in ((up, BY - 1, BY - 2), (down, 0, 1)):
        for x in range(BX):
            base = (x * BY + near) * ROWS
            ref[x * WIRE : (x + 1) * WIRE, :] = own[base : base + WIRE, :]
            base = (x * BY + next_) * ROWS
            start = BX * WIRE + x * NEAR
            ref[start : start + NEAR, :] = own[base : base + NEAR, :]


XMSG = BY * (WIRE + NEAR)
YMSG = BX * (WIRE + NEAR)
CMSG = 2 * WIRE + 6 * NEAR
XHALO = 8 * ROWS + 8 * NEAR


def corner_rows(ring, fx):
    if ring == 1:
        return {-1: 0, 3: WIRE, -2: 2 * WIRE, 4: 2 * WIRE + NEAR}[fx]
    return 2 * WIRE + 2 * NEAR + {-2: 0, -1: 1, 3: 2, 4: 3}[fx] * NEAR


def x_rows(fx, y):
    if fx in (-1, 3):
        return ((0 if fx < 0 else BY) + y) * ROWS
    return 8 * ROWS + ((0 if fx < 0 else BY) + y) * NEAR


def settle(src, base, dst, to, full, axis, move):
    for h in range(2):
        rho = src[base + 48 + 8 * h : base + 56 + 8 * h, :]
        for k in (0, 1, 2, 3, 5, 6, 7) if full else range(4):
            row = PART[k] + 8 * h
            value = src[base + row : base + row + 8, :]
            if k == axis:
                value = value + move
            if k == 0:
                value = jnp.where(rho > 0.0, value, FAR)
            dst[to + row : to + row + 8, :] = value
        if full:
            term = pressure_term(jnp.where(rho > 0.0, 2.0 * rho, 1.0))
            dst[to + 128 + 8 * h : to + 136 + 8 * h, :] = term
    if full:
        base, to = base + WALL, to + WALL
        mask = src[base + 12 : base + 16, :]
        for k in range(3):
            value = src[base + 4 * k : base + 4 * k + 4, :]
            if k == axis:
                value = value + move
            if k == 0:
                value = jnp.where(mask > 0.0, value, FAR)
            dst[to + 4 * k : to + 4 * k + 4, :] = value
        dst[to + 12 : to + 16, :] = mask


def forward_body(own, from_left, from_right, halo, up, down):
    for src, fx, fx2, move in ((from_left, -1, -2, -3.0), (from_right, 3, 4, 3.0)):
        for y in range(BY):
            settle(src, y * WIRE, halo, x_rows(fx, y), True, 0, move)
            settle(src, BY * WIRE + y * NEAR, halo, x_rows(fx2, y), False, 0, move)
    for ref, near, next_ in ((up, BY - 1, BY - 2), (down, 0, 1)):
        for ring, y in ((1, near), (2, next_)):
            for fx in (-2, -1, 3, 4):
                count = WIRE if (ring == 1 and fx in (-1, 3)) else NEAR
                to = corner_rows(ring, fx)
                base = x_rows(fx, y)
                ref[to : to + count, :] = halo[base : base + count, :]


def roll_columns(src, rolled, count):
    for q in range(count):
        for v, move in enumerate((-1, 1)):
            for k in range(8):
                for h in range(2):
                    base = q * ROWS + PART[k] + 8 * h
                    value = shifted(src[base : base + 8, :], move, PAD if k == 0 else None)
                    if k == 2:
                        value = value + float(move)
                    to = (v * count + q) * 128 + 16 * k + 8 * h
                    rolled[to : to + 8, :] = value


def own_body(count, selfs, tab, own, out, rolled, acc, racc):
    zero = jnp.zeros((8, 128), F32)

    def clear(i, c):
        base = i * 128
        for k in range(16):
            put8(acc, base + 8 * k, zero)
        return c

    lax.fori_loop(0, COLS * 4 * SLOTS * 8 // 128, clear, 0)

    def clear_r(i, c):
        for k in range(24):
            put8(racc, i * 192 + 8 * k, zero)
        return c

    lax.fori_loop(0, COLS, clear_r, 0)

    roll_columns(own, rolled, COLS)

    def block(t, s, v, symmetric):
        for h in range(2):
            if v == 0:
                src = [rows8(own, s * ROWS + PART[k] + 8 * h) for k in range(8)]
            else:
                src = [rows8(rolled, ((v - 1) * COLS + s) * 128 + 16 * k + 8 * h) for k in range(8)]
            back = [zero] * 4
            for i in range(SLOTS):
                dst = [spread(own, t * ROWS + PART[k] + i) for k in range(8)]
                terms = fluid_pair(dst, src)
                for c in range(4):
                    base = ((t * 4 + c) * SLOTS + i) * 8
                    put8(acc, base, rows8(acc, base) + terms[c])
                if symmetric:
                    for c in range(3):
                        back[c] = back[c] - terms[c]
                    back[3] = back[3] + terms[3]
            if symmetric:
                for c in range(4):
                    base = (s * 3 + v) * 64 + 16 * c + 8 * h
                    put8(racc, base, rows8(racc, base) + back[c])

    def pair(e, c):
        t, s = tab[0, e], tab[1, e]
        for v in range(3):
            block(t, s, v, True)
        return c

    lax.fori_loop(0, count, pair, 0)
    if selfs:

        def alone(q, c):
            block(q, q, 0, False)
            block(q, q, 2, True)
            return c

        lax.fori_loop(0, COLS, alone, 0)

    sub = lax.broadcasted_iota(jnp.int32, (8, 128), 0)

    def gather_rows(values):
        for bit in (1, 2, 4):
            odd = (sub & bit) != 0
            values = [
                jnp.where(odd, b, a) + pltpu.roll(jnp.where(odd, a, b), bit, 0) if bit == 4
                else jnp.where(odd, b + pltpu.roll(b, bit, 0), a + pltpu.roll(a, 8 - bit, 0))
                for a, b in zip(values[0::2], values[1::2])
            ]
        return values[0]

    def finish(group, c):
        for n in range(3):
            q = group * 3 + n
            for k in range(8):
                start = (q * 4 * SLOTS + 8 * k) * 8
                value = gather_rows([rows8(acc, start + 8 * i) for i in range(8)])
                value = value + rows8(racc, q * 192 + 8 * k)
                value = value + pltpu.roll(rows8(racc, q * 192 + 64 + 8 * k), 127, 1)
                value = value + pltpu.roll(rows8(racc, q * 192 + 128 + 8 * k), 1, 1)
                put8(out, q * 64 + 8 * k, value)
        return c

    lax.fori_loop(0, COLS // 3, finish, 0)


SIDES = (
    [(-1, y) for y in range(BY)]
    + [(BX, y) for y in range(BY)]
    + [(x, -1) for x in range(BX)]
    + [(x, BY) for x in range(BX)]
)
CORNERS = [(-1, -1), (BX, -1), (-1, BY), (BX, BY)]
FRAME = (BX + 4) * (BY + 4)
LOW = 16
ROOM = 64500000
MOVES = [(sx, sy) for sx in (-1, 0, 1) for sy in (-1, 0, 1)]


def frame(fx, fy):
    return (fx + 2) * 8 + fy + 2


def turn(value, shift):
    return pltpu.roll(value, shift % 128, 1) if shift % 128 else value


def against(own, q, h, sources, total, first=0, last=SLOTS):
    t = [rows8(own, q * ROWS + PART[k] + 8 * h) for k in range(8)]
    sums = [jnp.zeros((8, 128), F32)] * 4
    for ref, base, at in sources:
        for j in range(first, last):
            terms = fluid_pair(t, [spread(ref, base + at[k] + j) for k in range(8)])
            sums = [a + b for a, b in zip(sums, terms)]
    for c in range(4):
        base = q * 64 + 16 * c + 8 * h
        put8(total, base, rows8(total, base) + sums[c])


DENSE = tuple(16 * k for k in range(8))


def crowded(refs):
    least = jnp.full((8, 128), FAR, F32)
    for ref, base in refs:
        least = jnp.minimum(least, ref[base + 8 : base + 16, :])
    return jnp.min(least) < 0.5 * FAR


def sides_body(count, tab, own, halo, from_down, from_up, inner, near, total, rolled):
    for n, (fx, fy) in enumerate(SIDES):
        if 0 <= fy < BY:
            base = x_rows(fx, fy)
            near[n * ROWS : (n + 1) * ROWS, :] = halo[base : base + ROWS, :]
        else:
            src, move = (from_down, -4.0) if fy < 0 else (from_up, 4.0)
            settle(src, fx * WIRE, near, n * ROWS, True, 1, move)
    total[...] = inner[...]
    roll_columns(near, rolled, len(SIDES))
    many_own = crowded([(own, q * ROWS) for q in range(COLS)])
    many_near = crowded([(near, n * ROWS) for n in range(len(SIDES))])

    def pair(e, carry):
        q, n = tab[0, e], tab[1, e]
        sources = [(near, n * ROWS, PART)]
        sources += [(rolled, (v * len(SIDES) + n) * 128, DENSE) for v in range(2)]
        against(own, q, 0, sources, total, 0, 8)

        @pl.when(many_near)
        def _():
            against(own, q, 0, sources, total, 8, 16)

        @pl.when(many_own)
        def _():
            against(own, q, 1, sources, total, 0, 8)

        @pl.when(many_own & many_near)
        def _():
            against(own, q, 1, sources, total, 8, 16)

        return carry

    lax.fori_loop(0, count, pair, 0)


def sum_walls(spots, sources):
    zero = jnp.zeros((8, 128), F32)
    mass, load = [zero] * WALLS, [zero] * WALLS
    for get in sources:
        s = get()
        for w in range(WALLS):
            dz = spots[w][2] - s[2]
            value = weight(spots[w][0] - s[0], spots[w][1] - s[1], dz)
            mass[w] = mass[w] + value
            load[w] = load[w] + value * (s[4] - s[3] * dz)
    return [
        jnp.sum(load[w], axis=0, keepdims=True) / jnp.maximum(jnp.sum(mass[w], axis=0, keepdims=True), 1.0)
        for w in range(WALLS)
    ]


def rim_body(
    own, halo, near, down_side, up_side, down_corner, up_corner, part, acc_out, rate_out, top,
    corner, rolled, geo, walls, low_walls, total, bottom, target, wbot, wroll, rbot, stage,
    low_geo, low_wall, low_target, low_sum,
):
    zero = jnp.zeros((8, 128), F32)
    lane = lanes()
    sub = lax.broadcasted_iota(jnp.int32, (8, 128), 0)
    for n, (fx, fy) in enumerate(CORNERS):
        src, move = (down_corner, -4.0) if fy < 0 else (up_corner, 4.0)
        settle(src, corner_rows(1, fx), corner, n * ROWS, True, 1, move)
    total[...] = part[...]
    roll_columns(corner, rolled, len(CORNERS))
    for n, (fx, fy) in enumerate(CORNERS):
        q = min(max(fx, 0), BX - 1) * BY + min(max(fy, 0), BY - 1)
        sources = [(corner, n * ROWS, PART)]
        sources += [(rolled, (v * len(CORNERS) + n) * 128, DENSE) for v in range(2)]
        for h in range(2):
            against(own, q, h, sources, total)

    def place(fx, fy):
        if 0 <= fx < BX and 0 <= fy < BY:
            return own, (fx * BY + fy) * ROWS
        if (fx, fy) in SIDES:
            return near, SIDES.index((fx, fy)) * ROWS
        return corner, CORNERS.index((fx, fy)) * ROWS

    for fx in range(-2, BX + 2):
        for fy in range(-2, BY + 2):
            to = frame(fx, fy) * 80
            if -1 <= fx <= BX and -1 <= fy <= BY:
                ref, base = place(fx, fy)
            elif 0 <= fy < BY:
                ref, base = halo, x_rows(fx, fy)
            else:
                ring = 2 if fy in (-2, BY + 1) else 1
                move = -4.0 if fy < 0 else 4.0
                if 0 <= fx < BX:
                    src, base = (down_side if fy < 0 else up_side), BX * WIRE + fx * NEAR
                else:
                    src, base = (down_corner if fy < 0 else up_corner), corner_rows(ring, fx)
                settle(src, base, geo, to, False, 1, move)
                ref, base = geo, to
            for h in range(2):
                rho = 2.0 * ref[base + 48 + 8 * h : base + 56 + 8 * h, :]
                if ref is not geo:
                    for k in range(3):
                        row = 16 * k + 8 * h
                        geo[to + row : to + row + 8, :] = ref[base + row : base + row + 8, :]
                rho2 = rho * rho
                geo[to + 48 + 8 * h : to + 56 + 8 * h, :] = GRAVITY * rho
                geo[to + 64 + 8 * h : to + 72 + 8 * h, :] = STIFFNESS * ((rho2 * rho2) * (rho2 * rho) - 1.0)

    for k in range(10):
        low, high = zero, zero
        for h in range(FRAME):
            value = geo[h * 80 + 8 * k : h * 80 + 8 * k + 8, :]
            low = jnp.where(lane == h, turn(value, h), low)
            high = jnp.where(lane == h, turn(value, h - 1), high)
        bottom[8 * k : 8 * k + 8, :] = low
        bottom[80 + 8 * k : 88 + 8 * k, :] = high + 1.0 if k in (4, 5) else high
    for k in range(16):
        low, high = zero, zero
        for q in range(COLS):
            h = frame(*divmod(q, BY))
            base = q * ROWS + PART[k // 2] + 8 * (k % 2)
            value = own[base : base + 8, :]
            low = jnp.where(lane == h, turn(value, h), low)
            high = jnp.where(lane == h, turn(value, h - 1), high)
        target[8 * k : 8 * k + 8, :] = low
        target[128 + 8 * k : 136 + 8 * k, :] = high + 1.0 if k in (4, 5) else high
    codes = [zero] * 4
    wa, wb = zero, zero
    for n in range(30):
        fx, fy = n // 6 - 1, n % 6 - 1
        ref, base = place(fx, fy)
        base += WALL
        xy, zm = ref[base : base + 8, :], ref[base + 8 : base + 16, :]
        h = frame(fx, fy)
        wa = jnp.where(lane == h, turn(xy, h), wa)
        wb = jnp.where(lane == h, turn(zm, h), wb)
        mask = jnp.max(jnp.where(sub >= 4, zm, 0.0), axis=0, keepdims=True)
        one = lane[0:1]
        high = jnp.max(jnp.where(one >= LOW - 1, mask, 0.0), axis=1, keepdims=True)
        some = jnp.max(jnp.where((one >= 1) & (one < LOW - 1), mask, 0.0), axis=1, keepdims=True)
        some = jnp.where(high > 0.0, 0.0, some)
        bit = float(1 << (n % 15))
        g = 0 if n < 15 else 1
        codes[g] = codes[g] + jnp.where(high > 0.0, bit, 0.0)
        codes[2] = jnp.maximum(codes[2], some)
        walls[n * 16 : n * 16 + 8, :] = jnp.where((lane == 0) & (sub < 4), FAR, xy)
        walls[n * 16 + 8 : n * 16 + 16, :] = zm
        keep = jnp.broadcast_to(some > 0.0, (8, 128)) & (lane >= 1) & (lane < LOW - 1)
        low_walls[n * 8 : n * 8 + 8, :] = jnp.where((sub >= 4) | keep, xy, FAR)
    wbot[0:8, :] = wa
    wbot[8:16, :] = wb
    flags_a = jnp.max(codes[0]).astype(jnp.int32)
    flags_b = jnp.max(codes[1]).astype(jnp.int32)
    low_any = jnp.max(codes[2]) > 0.0

    def from_bottom(z, h, back):
        def get():
            base = 80 * z + 8 * h
            return [turn(bottom[base + 16 * k : base + 16 * k + 8, :], back) for k in range(5)]

        return get

    spots = [[spread(wbot, 4 * k + w) for k in range(3)] for w in range(WALLS)]
    found = sum_walls(spots, [from_bottom(z, h, -(sx * 8 + sy)) for sx, sy in MOVES for z in range(2) for h in range(2)])
    for w in range(WALLS):
        wbot[12 + w : 13 + w, :] = found[w]
    for m, (sx, sy) in enumerate(MOVES):
        for k in range(2):
            wroll[16 * m + 8 * k : 16 * m + 8 * k + 8, :] = turn(wbot[8 * k : 8 * k + 8, :], -(sx * 8 + sy))
    for z in range(2):
        for h in range(2):
            t = [target[128 * z + 16 * k + 8 * h : 128 * z + 16 * k + 8 * h + 8, :] for k in range(8)]
            t[3] = t[3] + 0.5
            sums = [zero] * 4
            for m in range(9):
                for w in range(WALLS):
                    terms = wall_pair(t, [spread(wroll, 16 * m + 4 * k + w) for k in range(4)])
                    sums = [a + b for a, b in zip(sums, terms)]
            for c in range(4):
                rbot[64 * z + 16 * c + 8 * h : 64 * z + 16 * c + 8 * h + 8, :] = sums[c]
    for q in range(COLS):
        h = frame(*divmod(q, BY))
        for k in range(8):
            base = q * 64 + 8 * k
            low = turn(rbot[8 * k : 8 * k + 8, :], -h)
            high = turn(rbot[64 + 8 * k : 72 + 8 * k, :], 1 - h)
            add = jnp.where(lane == 0, low, jnp.where(lane == 1, high, 0.0))
            total[base : base + 8, :] = total[base : base + 8, :] + add

    @pl.when(low_any)
    def _():
        block = lane // LOW
        for i in range(BX + 4):
            for k in range(10):
                value = zero
                for j in range(8):
                    base = (i * 8 + j) * 80 + 8 * k
                    value = jnp.where(block == j, turn(geo[base : base + 8, :], j * LOW), value)
                low_geo[i * 80 + 8 * k : i * 80 + 8 * k + 8, :] = value
        for i in range(BX + 2):
            xy, zm = jnp.where(sub < 4, FAR, zero), zero
            for j in range(6):
                n = i * 6 + j
                xy = jnp.where(block == j + 1, turn(low_walls[n * 8 : n * 8 + 8, :], (j + 1) * LOW), xy)
                zm = jnp.where(block == j + 1, turn(walls[n * 16 + 8 : n * 16 + 16, :], (j + 1) * LOW), zm)
            low_wall[i * 16 : i * 16 + 8, :] = xy
            low_wall[i * 16 + 8 : i * 16 + 16, :] = zm
        for i in range(BX):
            for k in range(16):
                value = zero
                for j in range(BY):
                    base = (i * BY + j) * ROWS + PART[k // 2] + 8 * (k % 2)
                    value = jnp.where(block == j + 2, turn(own[base : base + 8, :], (j + 2) * LOW), value)
                low_target[i * 128 + 8 * k : i * 128 + 8 * k + 8, :] = value
        steps = [(sx, sy, dz) for sx, sy in MOVES for dz in (-1, 0, 1)]

        def press(i, carry):
            for m, (sx, sy, dz) in enumerate(steps):
                for k in range(10):
                    value = turn(rows8(low_geo, (i + 1 + sx) * 80 + 8 * k), -(sy * LOW + dz))
                    if k in (4, 5) and dz:
                        value = value + float(dz)
                    stage[m * 80 + 8 * k : m * 80 + 8 * k + 8, :] = value

            def from_stage(m, h):
                return lambda: [stage[m * 80 + 16 * k + 8 * h : m * 80 + 16 * k + 8 * h + 8, :] for k in range(5)]

            spots = [[spread(low_wall, i * 16 + 4 * k + w) for k in range(3)] for w in range(WALLS)]
            found = sum_walls(spots, [from_stage(m, h) for m in range(27) for h in range(2)])
            for w in range(WALLS):
                low_wall[pl.ds(i * 16 + 12 + w, 1), :] = found[w]
            return carry

        lax.fori_loop(0, BX + 2, press, 0)

        def push(i, carry):
            for m, (sx, sy, dz) in enumerate(steps):
                for k in range(2):
                    value = turn(rows8(low_wall, (i + 1 + sx) * 16 + 8 * k), -(sy * LOW + dz))
                    if k == 1 and dz:
                        value = jnp.where(sub < 4, value + float(dz), value)
                    stage[m * 16 + 8 * k : m * 16 + 8 * k + 8, :] = value
            for h in range(2):
                t = [rows8(low_target, i * 128 + 16 * k + 8 * h) for k in range(8)]
                t[3] = t[3] + 0.5
                sums = [zero] * 4
                for m in range(27):
                    for w in range(WALLS):
                        terms = wall_pair(t, [spread(stage, 16 * m + 4 * k + w) for k in range(4)])
                        sums = [a + b for a, b in zip(sums, terms)]
                for c in range(4):
                    put8(low_sum, i * 64 + 16 * c + 8 * h, sums[c])
            return carry

        lax.fori_loop(0, BX, push, 0)
        for i in range(BX):
            for j in range(BY):
                for k in range(8):
                    base = (i * BY + j) * 64 + 8 * k
                    add = turn(low_sum[i * 64 + 8 * k : i * 64 + 8 * k + 8, :], -(j + 2) * LOW)
                    total[base : base + 8, :] = total[base : base + 8, :] + jnp.where(lane < LOW, add, 0.0)

    def wall_column(n, carry):
        flag = jnp.where(n < 15, flags_a >> jnp.minimum(n, 15), flags_b >> jnp.maximum(n - 15, 0)) & 1

        @pl.when(flag == 1)
        def _():
            kx, ky = n // 6, n % 6
            for m, (sx, sy) in enumerate(MOVES):
                h = (kx + 1 + sx) * 8 + ky + 1 + sy
                for k in range(10):
                    value = rows8(geo, h * 80 + 8 * k)
                    for v, move in enumerate((-1, 1)):
                        moved = shifted(value, move, PAD if k < 2 else None)
                        if k in (4, 5):
                            moved = moved + float(move)
                        stage[(v * 9 + m) * 80 + 8 * k : (v * 9 + m) * 80 + 8 * k + 8, :] = moved

            def from_stage(m, v, j):
                def get():
                    if v == 0:
                        h = (kx + 1 + MOVES[m][0]) * 8 + ky + 1 + MOVES[m][1]
                        return [rows8(geo, h * 80 + 16 * k + 8 * j) for k in range(5)]
                    base = ((v - 1) * 9 + m) * 80 + 8 * j
                    return [stage[base + 16 * k : base + 16 * k + 8, :] for k in range(5)]

                return get

            spots = [[spread(walls, n * 16 + 4 * k + w) for k in range(3)] for w in range(WALLS)]
            found = sum_walls(spots, [from_stage(m, v, j) for m in range(9) for v in range(3) for j in range(2)])
            for w in range(WALLS):
                walls[pl.ds(n * 16 + 12 + w, 1), :] = found[w]
            for v, move in enumerate((0, -1, 1)):
                for k in range(2):
                    value = rows8(walls, n * 16 + 8 * k)
                    if move:
                        moved = turn(value, -move)
                        if k == 0:
                            edge = lane == (127 if move > 0 else 0)
                            value = jnp.where(edge & (sub < 4), FAR, moved)
                        else:
                            value = jnp.where(sub < 4, moved + float(move), moved)
                    stage[v * 16 + 8 * k : v * 16 + 8 * k + 8, :] = value

            def over_x(x, c):
                def over_y(y, c):
                    q = x * BY + y
                    for h in range(2):
                        t = [rows8(own, q * ROWS + PART[k] + 8 * h) for k in range(8)]
                        t[3] = t[3] + 0.5
                        sums = [zero] * 4
                        for v in range(3):
                            for w in range(WALLS):
                                terms = wall_pair(t, [spread(stage, v * 16 + 4 * k + w) for k in range(4)])
                                sums = [a + b for a, b in zip(sums, terms)]
                        for c4 in range(4):
                            base = q * 64 + 16 * c4 + 8 * h
                            put8(total, base, rows8(total, base) + sums[c4])
                    return c

                return lax.fori_loop(jnp.maximum(ky - 2, 0), jnp.minimum(ky, BY - 1) + 1, over_y, c)

            lax.fori_loop(jnp.maximum(kx - 2, 0), jnp.minimum(kx, BX - 1) + 1, over_x, 0)

        return carry

    @pl.when(flags_a + flags_b > 0)
    def _():
        lax.fori_loop(0, 30, wall_column, 0)

    most = jnp.zeros((SLOTS, 128), F32)
    for q in range(COLS):
        live = own[q * ROWS : q * ROWS + 16, :] < 0.5 * FAR
        sq = jnp.zeros((SLOTS, 128), F32)
        for c in range(3):
            value = SCALE * total[q * 64 + 16 * c : q * 64 + 16 * c + 16, :]
            if c == 2:
                value = value - GRAVITY
            value = jnp.where(live, value, 0.0)
            sq = sq + value * value
            acc_out[pl.ds(c * SLOTS * COLS + q, SLOTS, stride=COLS), :] = value
        most = jnp.maximum(most, sq)
        rate = -SCALE * total[q * 64 + 48 : q * 64 + 64, :]
        rate_out[pl.ds(q, SLOTS, stride=COLS), :] = jnp.where(live, rate, 0.0)
    top[...] = jnp.zeros(top.shape, F32) + jnp.max(most)


def shape(*dims):
    return jax.ShapeDtypeStruct(dims, F32)


def vmem(rows):
    return pltpu.VMEM((rows, 128), F32)


def call(body, outs, operands, scratch=(), flops=0, tables=0, name=None, space=pltpu.VMEM, room=48 << 20):
    specs = [pl.BlockSpec(memory_space=pltpu.SMEM)] * tables
    specs += [pl.BlockSpec(memory_space=space)] * (len(operands) - tables)
    return pl.pallas_call(
        body,
        out_shape=outs,
        in_specs=specs,
        out_specs=jax.tree.map(lambda _: pl.BlockSpec(memory_space=pltpu.VMEM), outs),
        scratch_shapes=list(scratch),
        cost_estimate=pl.CostEstimate(flops=flops, transcendentals=0, bytes_accessed=1000000),
        compiler_params=pltpu.CompilerParams(vmem_limit_bytes=room),
        name=name,
    )(*operands)


def tables():
    inner, outer = [], []
    for q in range(COLS):
        x, y = divmod(q, BY)
        for sx, sy in MOVES:
            nx, ny = x + sx, y + sy
            if 0 <= nx < BX and 0 <= ny < BY:
                if nx * BY + ny > q:
                    inner.append((q, nx * BY + ny))
            elif (nx, ny) in SIDES:
                outer.append((q, SIDES.index((nx, ny))))
    return np.array(inner, np.int32).T.copy(), np.array(outer, np.int32).T.copy()


def on_device(fluid_offsets, fluid_velocity, fluid_density, fluid_counts, wall_offsets, wall_counts):
    flat = lambda a: a.reshape(-1, 128)
    inner, outer = tables()
    inner_table, outer_table = jnp.asarray(inner), jnp.asarray(outer)
    counts = pltpu.VMEM((BX, BY, 128), jnp.int32)
    own, right, left, up, down = call(
        pack_body,
        (shape(COLS * ROWS, 128), shape(XMSG, 128), shape(XMSG, 128), shape(YMSG, 128), shape(YMSG, 128)),
        (flat(fluid_offsets), flat(fluid_velocity), flat(fluid_density), fluid_counts, flat(wall_offsets), wall_counts),
        (vmem(576), vmem(576), vmem(192), counts, vmem(144), counts, pltpu.SemaphoreType.DMA((6,))),
        space=pltpu.HBM, room=ROOM, name="pack",
    )

    def ring(axis, step):
        size = lax.axis_size(axis)
        return [(i, i + step) for i in range(size) if 0 <= i + step < size]

    def exchange(axis, onward, backward):
        return lax.ppermute(onward, axis, ring(axis, 1)), lax.ppermute(backward, axis, ring(axis, -1))

    down_side, up_side = exchange(YZ, up, down)
    from_left, from_right = exchange(GX, right, left)
    part = call(
        partial(own_body, inner.shape[1], True), shape(COLS * 64, 128), (inner_table, own),
        (vmem(2 * COLS * 128), vmem(COLS * 4 * SLOTS * 8), vmem(COLS * 3 * 64)),
        flops=60000000, tables=1, name="inner",
    )
    down_side, up_side, from_left, from_right, part = lax.optimization_barrier(
        (down_side, up_side, from_left, from_right, part)
    )
    halo, corner_up, corner_down = call(
        forward_body, (shape(XHALO, 128), shape(CMSG, 128), shape(CMSG, 128)),
        (own, from_left, from_right), name="forward",
    )
    down_corner, up_corner = exchange(YZ, corner_up, corner_down)
    near, part = call(
        partial(sides_body, outer.shape[1]), (shape(len(SIDES) * ROWS, 128), shape(COLS * 64, 128)),
        (outer_table, own, halo, down_side, up_side, part), (vmem(2 * len(SIDES) * 128),),
        flops=60000000, tables=1, name="sides",
    )
    part, down_corner, up_corner = lax.optimization_barrier((part, down_corner, up_corner))
    acc, rate, top = call(
        rim_body,
        (shape(3 * SLOTS * COLS, 128), shape(SLOTS * COLS, 128), shape(8, 128)),
        (own, halo, near, down_side, up_side, down_corner, up_corner, part),
        (
            vmem(4 * ROWS), vmem(2 * 4 * 128), vmem(FRAME * 80), vmem(30 * 16), vmem(30 * 8), vmem(COLS * 64),
            vmem(160), vmem(256), vmem(16), vmem(144), vmem(128), vmem(27 * 80),
            vmem(7 * 80), vmem(5 * 16), vmem(3 * 128), vmem(3 * 64),
        ),
        name="rim",
    )
    devices = lax.axis_size(GX + YZ)
    tops = lax.all_to_all(jnp.broadcast_to(top[:1][None], (devices, 1, 128)), GX + YZ, 0, 0, tiled=True)
    largest = jnp.max(tops)
    step = 0.25 * jnp.sqrt(0.5 / (jnp.sqrt(largest) + 1e-6))
    return step * acc.reshape(fluid_offsets.shape), rate.reshape(fluid_density.shape)


def solution(mesh):
    gx, yz = GX, YZ
    split = Mesh(mesh.devices.reshape(4, 2, 2, 4, 4), GX + YZ)
    placed = (
        P(None, None, gx, yz, None),
        P(None, None, gx, yz, None),
        P(None, gx, yz, None),
        P(gx, yz, None),
        P(None, None, gx, yz, None),
        P(gx, yz, None),
    )
    return jax.shard_map(
        on_device,
        mesh=split,
        in_specs=placed,
        out_specs=(P(None, None, gx, yz, None), P(None, gx, yz, None)),
        check_vma=False,
    )
```

```python
from functools import partial

import jax
import jax.numpy as jnp
import numpy as np
from jax import lax
from jax.experimental import pallas as pl
from jax.experimental.pallas import tpu as pltpu
from jax.sharding import Mesh
from jax.sharding import PartitionSpec as P

GX = ("gx_0", "gx_1", "gx_2")
YZ = ("yz_0", "yz_1")

GRAVITY = 2.0
STIFFNESS = 100.0 / 7.0
SOFT = 0.0025
SCALE = 2.5
FAR = 1.0e6
PAD = -1.0e6
BX, BY, SLOTS, WALLS = 3, 4, 16, 4
COLS = BX * BY
ROWS = 144
WIRE = 128
NEAR = 64
WALL = 112
PART = (0, 16, 32, 48, 128, 64, 80, 96)
F32 = jnp.float32


def rows8(ref, base):
    return ref[pl.ds(pl.multiple_of(base, 8), 8), :]


def spread(ref, row):
    return ref[pl.ds(row, 8, stride=0), :]


def put8(ref, base, value):
    ref[pl.ds(pl.multiple_of(base, 8), 8), :] = value


def lanes():
    return lax.broadcasted_iota(jnp.int32, (8, 128), 1)


def shifted(value, move, fill=None):
    out = pltpu.roll(value, (-move) % 128, 1)
    if fill is None:
        return out
    return jnp.where(lanes() == (127 if move > 0 else 0), fill, out)


def slope(dx, dy, dz):
    squared = dx * dx + dy * dy + dz * dz
    distance = pl.reciprocal(lax.rsqrt(squared), approx=True)
    remain = jnp.maximum(1.0 - distance, 0.0)
    return squared, remain * remain * remain


def weight(dx, dy, dz):
    squared = dx * dx + dy * dy + dz * dz
    distance = pl.reciprocal(lax.rsqrt(squared), approx=True)
    remain = jnp.maximum(1.0 - distance, 0.0)
    twice = remain * remain
    return (twice * twice) * (4.0 * distance + 1.0)


def fluid_pair(t, s):
    dx, dy, dz = t[0] - s[0], t[1] - s[1], t[2] - s[2]
    squared, cube = slope(dx, dy, dz)
    approach = (t[5] - s[5]) * dx + (t[6] - s[6]) * dy + (t[7] - s[7]) * dz
    below = (squared + SOFT) * (t[3] + s[3])
    viscous = jnp.minimum(approach, 0.0) * pl.reciprocal(below, approx=True)
    factor = cube * ((t[4] + s[4]) - viscous)
    return factor * dx, factor * dy, factor * dz, cube * approach


def wall_pair(t, s):
    dx, dy, dz = t[0] - s[0], t[1] - s[1], t[2] - s[2]
    squared, cube = slope(dx, dy, dz)
    approach = t[5] * dx + t[6] * dy + t[7] * dz
    below = (squared + SOFT) * t[3]
    viscous = jnp.minimum(approach, 0.0) * pl.reciprocal(below, approx=True)
    factor = cube * ((t[4] + s[3]) - viscous)
    return factor * dx, factor * dy, factor * dz, cube * approach


def pressure_term(rho):
    rho2 = rho * rho
    return (STIFFNESS * ((rho2 * rho2) * (rho2 * rho) - 1.0)) / rho2


def pack_body(
    off_in, vel_in, den_in, cnt_in, woff_in, wcnt_in, own, right, left, up, down,
    off, vel, den, cnt, woff, wcnt, sems,
):
    copies = [
        pltpu.make_async_copy(src, dst, sems.at[n])
        for n, (src, dst) in enumerate(
            zip((off_in, vel_in, den_in, cnt_in, woff_in, wcnt_in), (off, vel, den, cnt, woff, wcnt))
        )
    ]
    for copy in copies:
        copy.start()
    for copy in copies:
        copy.wait()
    slot = lax.broadcasted_iota(jnp.int32, (SLOTS, 128), 0)
    wslot = lax.broadcasted_iota(jnp.int32, (WALLS, 128), 0)
    for q in range(COLS):
        x, y = divmod(q, BY)
        base = q * ROWS
        live = slot < jnp.broadcast_to(cnt[x, y : y + 1, :], (SLOTS, 128))

        def take(ref, part):
            return ref[pl.ds(part * SLOTS * COLS + q, SLOTS, stride=COLS), :]

        rho = take(den, 0)
        parts = (
            jnp.where(live, take(off, 0) + float(x), FAR),
            take(off, 1) + float(y),
            take(off, 2),
            0.5 * rho,
            pressure_term(rho),
            take(vel, 0),
            take(vel, 1),
            take(vel, 2),
        )
        for at, part in zip(PART, parts):
            own[base + at : base + at + 16, :] = part
        live = wslot < jnp.broadcast_to(wcnt[x, y : y + 1, :], (WALLS, 128))

        def wtake(part):
            return woff[pl.ds(part * WALLS * COLS + q, WALLS, stride=COLS), :]

        base += WALL
        own[base : base + 4, :] = jnp.where(live, wtake(0) + float(x), FAR)
        own[base + 4 : base + 8, :] = wtake(1) + float(y)
        own[base + 8 : base + 12, :] = wtake(2)
        own[base + 12 : base + 16, :] = jnp.where(live, 1.0, 0.0)
    for ref, first in ((right, BX - 1), (left, 0)):
        for y in range(BY):
            base = (first * BY + y) * ROWS
            ref[y * WIRE : (y + 1) * WIRE, :] = own[base : base + WIRE, :]
            base = (1 * BY + y) * ROWS
            start = BY * WIRE + y * NEAR
            ref[start : start + NEAR, :] = own[base : base + NEAR, :]
    for ref, near, next_ in ((up, BY - 1, BY - 2), (down, 0, 1)):
        for x in range(BX):
            base = (x * BY + near) * ROWS
            ref[x * WIRE : (x + 1) * WIRE, :] = own[base : base + WIRE, :]
            base = (x * BY + next_) * ROWS
            start = BX * WIRE + x * NEAR
            ref[start : start + NEAR, :] = own[base : base + NEAR, :]


XMSG = BY * (WIRE + NEAR)
YMSG = BX * (WIRE + NEAR)
CMSG = 2 * WIRE + 6 * NEAR
XHALO = 8 * ROWS + 8 * NEAR


def corner_rows(ring, fx):
    if ring == 1:
        return {-1: 0, 3: WIRE, -2: 2 * WIRE, 4: 2 * WIRE + NEAR}[fx]
    return 2 * WIRE + 2 * NEAR + {-2: 0, -1: 1, 3: 2, 4: 3}[fx] * NEAR


def x_rows(fx, y):
    if fx in (-1, 3):
        return ((0 if fx < 0 else BY) + y) * ROWS
    return 8 * ROWS + ((0 if fx < 0 else BY) + y) * NEAR


def settle(src, base, dst, to, full, axis, move):
    for h in range(2):
        rho = src[base + 48 + 8 * h : base + 56 + 8 * h, :]
        for k in (0, 1, 2, 3, 5, 6, 7) if full else range(4):
            row = PART[k] + 8 * h
            value = src[base + row : base + row + 8, :]
            if k == axis:
                value = value + move
            if k == 0:
                value = jnp.where(rho > 0.0, value, FAR)
            dst[to + row : to + row + 8, :] = value
        if full:
            term = pressure_term(jnp.where(rho > 0.0, 2.0 * rho, 1.0))
            dst[to + 128 + 8 * h : to + 136 + 8 * h, :] = term
    if full:
        base, to = base + WALL, to + WALL
        mask = src[base + 12 : base + 16, :]
        for k in range(3):
            value = src[base + 4 * k : base + 4 * k + 4, :]
            if k == axis:
                value = value + move
            if k == 0:
                value = jnp.where(mask > 0.0, value, FAR)
            dst[to + 4 * k : to + 4 * k + 4, :] = value
        dst[to + 12 : to + 16, :] = mask


def forward_body(own, from_left, from_right, halo, up, down):
    for src, fx, fx2, move in ((from_left, -1, -2, -3.0), (from_right, 3, 4, 3.0)):
        for y in range(BY):
            settle(src, y * WIRE, halo, x_rows(fx, y), True, 0, move)
            settle(src, BY * WIRE + y * NEAR, halo, x_rows(fx2, y), False, 0, move)
    for ref, near, next_ in ((up, BY - 1, BY - 2), (down, 0, 1)):
        for ring, y in ((1, near), (2, next_)):
            for fx in (-2, -1, 3, 4):
                count = WIRE if (ring == 1 and fx in (-1, 3)) else NEAR
                to = corner_rows(ring, fx)
                base = x_rows(fx, y)
                ref[to : to + count, :] = halo[base : base + count, :]


def roll_columns(src, rolled, count):
    for q in range(count):
        for v, move in enumerate((-1, 1)):
            for k in range(8):
                for h in range(2):
                    base = q * ROWS + PART[k] + 8 * h
                    value = shifted(src[base : base + 8, :], move, PAD if k == 0 else None)
                    if k == 2:
                        value = value + float(move)
                    to = (v * count + q) * 128 + 16 * k + 8 * h
                    rolled[to : to + 8, :] = value


def own_body(count, selfs, tab, own, out, rolled, acc, racc):
    zero = jnp.zeros((8, 128), F32)

    def clear(i, c):
        base = i * 128
        for k in range(16):
            put8(acc, base + 8 * k, zero)
        return c

    lax.fori_loop(0, COLS * 4 * SLOTS * 8 // 128, clear, 0)

    def clear_r(i, c):
        for k in range(24):
            put8(racc, i * 192 + 8 * k, zero)
        return c

    lax.fori_loop(0, COLS, clear_r, 0)

    roll_columns(own, rolled, COLS)

    def block(t, s, v, symmetric):
        for h in range(2):
            if v == 0:
                src = [rows8(own, s * ROWS + PART[k] + 8 * h) for k in range(8)]
            else:
                src = [rows8(rolled, ((v - 1) * COLS + s) * 128 + 16 * k + 8 * h) for k in range(8)]
            back = [zero] * 4
            for i in range(SLOTS):
                dst = [spread(own, t * ROWS + PART[k] + i) for k in range(8)]
                terms = fluid_pair(dst, src)
                for c in range(4):
                    base = ((t * 4 + c) * SLOTS + i) * 8
                    put8(acc, base, rows8(acc, base) + terms[c])
                if symmetric:
                    for c in range(3):
                        back[c] = back[c] - terms[c]
                    back[3] = back[3] + terms[3]
            if symmetric:
                for c in range(4):
                    base = (s * 3 + v) * 64 + 16 * c + 8 * h
                    put8(racc, base, rows8(racc, base) + back[c])

    def pair(e, c):
        t, s = tab[0, e], tab[1, e]
        for v in range(3):
            block(t, s, v, True)
        return c

    lax.fori_loop(0, count, pair, 0)
    if selfs:

        def alone(q, c):
            block(q, q, 0, False)
            block(q, q, 2, True)
            return c

        lax.fori_loop(0, COLS, alone, 0)

    sub = lax.broadcasted_iota(jnp.int32, (8, 128), 0)

    def gather_rows(values):
        for bit in (1, 2, 4):
            odd = (sub & bit) != 0
            values = [
                jnp.where(odd, b, a) + pltpu.roll(jnp.where(odd, a, b), bit, 0) if bit == 4
                else jnp.where(odd, b + pltpu.roll(b, bit, 0), a + pltpu.roll(a, 8 - bit, 0))
                for a, b in zip(values[0::2], values[1::2])
            ]
        return values[0]

    def finish(group, c):
        for n in range(3):
            q = group * 3 + n
            for k in range(8):
                start = (q * 4 * SLOTS + 8 * k) * 8
                value = gather_rows([rows8(acc, start + 8 * i) for i in range(8)])
                value = value + rows8(racc, q * 192 + 8 * k)
                value = value + pltpu.roll(rows8(racc, q * 192 + 64 + 8 * k), 127, 1)
                value = value + pltpu.roll(rows8(racc, q * 192 + 128 + 8 * k), 1, 1)
                put8(out, q * 64 + 8 * k, value)
        return c

    lax.fori_loop(0, COLS // 3, finish, 0)


SIDES = (
    [(-1, y) for y in range(BY)]
    + [(BX, y) for y in range(BY)]
    + [(x, -1) for x in range(BX)]
    + [(x, BY) for x in range(BX)]
)
CORNERS = [(-1, -1), (BX, -1), (-1, BY), (BX, BY)]
FRAME = (BX + 4) * (BY + 4)
LOW = 16
ROOM = 64500000
MOVES = [(sx, sy) for sx in (-1, 0, 1) for sy in (-1, 0, 1)]


def frame(fx, fy):
    return (fx + 2) * 8 + fy + 2


def turn(value, shift):
    return pltpu.roll(value, shift % 128, 1) if shift % 128 else value


def against(own, q, h, sources, total, first=0, last=SLOTS):
    t = [rows8(own, q * ROWS + PART[k] + 8 * h) for k in range(8)]
    sums = [jnp.zeros((8, 128), F32)] * 4
    for ref, base, at in sources:
        for j in range(first, last):
            terms = fluid_pair(t, [spread(ref, base + at[k] + j) for k in range(8)])
            sums = [a + b for a, b in zip(sums, terms)]
    for c in range(4):
        base = q * 64 + 16 * c + 8 * h
        put8(total, base, rows8(total, base) + sums[c])


DENSE = tuple(16 * k for k in range(8))


def crowded(refs):
    least = jnp.full((8, 128), FAR, F32)
    for ref, base in refs:
        least = jnp.minimum(least, ref[base + 8 : base + 16, :])
    return jnp.min(least) < 0.5 * FAR


def sides_body(count, tab, own, halo, from_down, from_up, inner, near, total, rolled):
    for n, (fx, fy) in enumerate(SIDES):
        if 0 <= fy < BY:
            base = x_rows(fx, fy)
            near[n * ROWS : (n + 1) * ROWS, :] = halo[base : base + ROWS, :]
        else:
            src, move = (from_down, -4.0) if fy < 0 else (from_up, 4.0)
            settle(src, fx * WIRE, near, n * ROWS, True, 1, move)
    total[...] = inner[...]
    roll_columns(near, rolled, len(SIDES))
    many_own = crowded([(own, q * ROWS) for q in range(COLS)])
    many_near = crowded([(near, n * ROWS) for n in range(len(SIDES))])

    def pair(e, carry):
        q, n = tab[0, e], tab[1, e]
        sources = [(near, n * ROWS, PART)]
        sources += [(rolled, (v * len(SIDES) + n) * 128, DENSE) for v in range(2)]
        for h in range(2):
            against(own, q, h, sources, total)
        return carry

    def sparse_pair(e, carry):
        q, n = tab[0, e], tab[1, e]
        sources = [(near, n * ROWS, PART)]
        sources += [(rolled, (v * len(SIDES) + n) * 128, DENSE) for v in range(2)]
        against(own, q, 0, sources, total, 0, 8)
        return carry

    few = jnp.logical_not(many_own | many_near)

    @pl.when(few)
    def _():
        lax.fori_loop(0, count, sparse_pair, 0)

    @pl.when(jnp.logical_not(few))
    def _():
        lax.fori_loop(0, count, pair, 0)


def sum_walls(spots, sources):
    zero = jnp.zeros((8, 128), F32)
    mass, load = [zero] * WALLS, [zero] * WALLS
    for get in sources:
        s = get()
        for w in range(WALLS):
            dz = spots[w][2] - s[2]
            value = weight(spots[w][0] - s[0], spots[w][1] - s[1], dz)
            mass[w] = mass[w] + value
            load[w] = load[w] + value * (s[4] - s[3] * dz)
    return [
        jnp.sum(load[w], axis=0, keepdims=True) / jnp.maximum(jnp.sum(mass[w], axis=0, keepdims=True), 1.0)
        for w in range(WALLS)
    ]


def rim_body(
    own, halo, near, down_side, up_side, down_corner, up_corner, part, acc_out, rate_out, top,
    corner, rolled, geo, walls, low_walls, total, bottom, target, wbot, wroll, rbot, stage,
    low_geo, low_wall, low_target, low_sum,
):
    zero = jnp.zeros((8, 128), F32)
    lane = lanes()
    sub = lax.broadcasted_iota(jnp.int32, (8, 128), 0)
    for n, (fx, fy) in enumerate(CORNERS):
        src, move = (down_corner, -4.0) if fy < 0 else (up_corner, 4.0)
        settle(src, corner_rows(1, fx), corner, n * ROWS, True, 1, move)
    total[...] = part[...]
    roll_columns(corner, rolled, len(CORNERS))
    for n, (fx, fy) in enumerate(CORNERS):
        q = min(max(fx, 0), BX - 1) * BY + min(max(fy, 0), BY - 1)
        sources = [(corner, n * ROWS, PART)]
        sources += [(rolled, (v * len(CORNERS) + n) * 128, DENSE) for v in range(2)]
        for h in range(2):
            against(own, q, h, sources, total)

    def place(fx, fy):
        if 0 <= fx < BX and 0 <= fy < BY:
            return own, (fx * BY + fy) * ROWS
        if (fx, fy) in SIDES:
            return near, SIDES.index((fx, fy)) * ROWS
        return corner, CORNERS.index((fx, fy)) * ROWS

    for fx in range(-2, BX + 2):
        for fy in range(-2, BY + 2):
            to = frame(fx, fy) * 80
            if -1 <= fx <= BX and -1 <= fy <= BY:
                ref, base = place(fx, fy)
            elif 0 <= fy < BY:
                ref, base = halo, x_rows(fx, fy)
            else:
                ring = 2 if fy in (-2, BY + 1) else 1
                move = -4.0 if fy < 0 else 4.0
                if 0 <= fx < BX:
                    src, base = (down_side if fy < 0 else up_side), BX * WIRE + fx * NEAR
                else:
                    src, base = (down_corner if fy < 0 else up_corner), corner_rows(ring, fx)
                settle(src, base, geo, to, False, 1, move)
                ref, base = geo, to
            for h in range(2):
                rho = 2.0 * ref[base + 48 + 8 * h : base + 56 + 8 * h, :]
                if ref is not geo:
                    for k in range(3):
                        row = 16 * k + 8 * h
                        geo[to + row : to + row + 8, :] = ref[base + row : base + row + 8, :]
                rho2 = rho * rho
                geo[to + 48 + 8 * h : to + 56 + 8 * h, :] = GRAVITY * rho
                geo[to + 64 + 8 * h : to + 72 + 8 * h, :] = STIFFNESS * ((rho2 * rho2) * (rho2 * rho) - 1.0)

    for k in range(10):
        low, high = zero, zero
        for h in range(FRAME):
            value = geo[h * 80 + 8 * k : h * 80 + 8 * k + 8, :]
            low = jnp.where(lane == h, turn(value, h), low)
            high = jnp.where(lane == h, turn(value, h - 1), high)
        bottom[8 * k : 8 * k + 8, :] = low
        bottom[80 + 8 * k : 88 + 8 * k, :] = high + 1.0 if k in (4, 5) else high
    for k in range(16):
        low, high = zero, zero
        for q in range(COLS):
            h = frame(*divmod(q, BY))
            base = q * ROWS + PART[k // 2] + 8 * (k % 2)
            value = own[base : base + 8, :]
            low = jnp.where(lane == h, turn(value, h), low)
            high = jnp.where(lane == h, turn(value, h - 1), high)
        target[8 * k : 8 * k + 8, :] = low
        target[128 + 8 * k : 136 + 8 * k, :] = high + 1.0 if k in (4, 5) else high
    codes = [zero] * 4
    wa, wb = zero, zero
    for n in range(30):
        fx, fy = n // 6 - 1, n % 6 - 1
        ref, base = place(fx, fy)
        base += WALL
        xy, zm = ref[base : base + 8, :], ref[base + 8 : base + 16, :]
        h = frame(fx, fy)
        wa = jnp.where(lane == h, turn(xy, h), wa)
        wb = jnp.where(lane == h, turn(zm, h), wb)
        mask = jnp.max(jnp.where(sub >= 4, zm, 0.0), axis=0, keepdims=True)
        one = lane[0:1]
        high = jnp.max(jnp.where(one >= LOW - 1, mask, 0.0), axis=1, keepdims=True)
        some = jnp.max(jnp.where((one >= 1) & (one < LOW - 1), mask, 0.0), axis=1, keepdims=True)
        some = jnp.where(high > 0.0, 0.0, some)
        bit = float(1 << (n % 15))
        g = 0 if n < 15 else 1
        codes[g] = codes[g] + jnp.where(high > 0.0, bit, 0.0)
        codes[2] = jnp.maximum(codes[2], some)
        walls[n * 16 : n * 16 + 8, :] = jnp.where((lane == 0) & (sub < 4), FAR, xy)
        walls[n * 16 + 8 : n * 16 + 16, :] = zm
        keep = jnp.broadcast_to(some > 0.0, (8, 128)) & (lane >= 1) & (lane < LOW - 1)
        low_walls[n * 8 : n * 8 + 8, :] = jnp.where((sub >= 4) | keep, xy, FAR)
    wbot[0:8, :] = wa
    wbot[8:16, :] = wb
    flags_a = jnp.max(codes[0]).astype(jnp.int32)
    flags_b = jnp.max(codes[1]).astype(jnp.int32)
    low_any = jnp.max(codes[2]) > 0.0

    def from_bottom(z, h, back):
        def get():
            base = 80 * z + 8 * h
            return [turn(bottom[base + 16 * k : base + 16 * k + 8, :], back) for k in range(5)]

        return get

    spots = [[spread(wbot, 4 * k + w) for k in range(3)] for w in range(WALLS)]
    found = sum_walls(spots, [from_bottom(z, h, -(sx * 8 + sy)) for sx, sy in MOVES for z in range(2) for h in range(2)])
    for w in range(WALLS):
        wbot[12 + w : 13 + w, :] = found[w]
    for m, (sx, sy) in enumerate(MOVES):
        for k in range(2):
            wroll[16 * m + 8 * k : 16 * m + 8 * k + 8, :] = turn(wbot[8 * k : 8 * k + 8, :], -(sx * 8 + sy))
    for z in range(2):
        for h in range(2):
            t = [target[128 * z + 16 * k + 8 * h : 128 * z + 16 * k + 8 * h + 8, :] for k in range(8)]
            t[3] = t[3] + 0.5
            sums = [zero] * 4
            for m in range(9):
                for w in range(WALLS):
                    terms = wall_pair(t, [spread(wroll, 16 * m + 4 * k + w) for k in range(4)])
                    sums = [a + b for a, b in zip(sums, terms)]
            for c in range(4):
                rbot[64 * z + 16 * c + 8 * h : 64 * z + 16 * c + 8 * h + 8, :] = sums[c]
    for q in range(COLS):
        h = frame(*divmod(q, BY))
        for k in range(8):
            base = q * 64 + 8 * k
            low = turn(rbot[8 * k : 8 * k + 8, :], -h)
            high = turn(rbot[64 + 8 * k : 72 + 8 * k, :], 1 - h)
            add = jnp.where(lane == 0, low, jnp.where(lane == 1, high, 0.0))
            total[base : base + 8, :] = total[base : base + 8, :] + add

    @pl.when(low_any)
    def _():
        block = lane // LOW
        for i in range(BX + 4):
            for k in range(10):
                value = zero
                for j in range(8):
                    base = (i * 8 + j) * 80 + 8 * k
                    value = jnp.where(block == j, turn(geo[base : base + 8, :], j * LOW), value)
                low_geo[i * 80 + 8 * k : i * 80 + 8 * k + 8, :] = value
        for i in range(BX + 2):
            xy, zm = jnp.where(sub < 4, FAR, zero), zero
            for j in range(6):
                n = i * 6 + j
                xy = jnp.where(block == j + 1, turn(low_walls[n * 8 : n * 8 + 8, :], (j + 1) * LOW), xy)
                zm = jnp.where(block == j + 1, turn(walls[n * 16 + 8 : n * 16 + 16, :], (j + 1) * LOW), zm)
            low_wall[i * 16 : i * 16 + 8, :] = xy
            low_wall[i * 16 + 8 : i * 16 + 16, :] = zm
        for i in range(BX):
            for k in range(16):
                value = zero
                for j in range(BY):
                    base = (i * BY + j) * ROWS + PART[k // 2] + 8 * (k % 2)
                    value = jnp.where(block == j + 2, turn(own[base : base + 8, :], (j + 2) * LOW), value)
                low_target[i * 128 + 8 * k : i * 128 + 8 * k + 8, :] = value
        steps = [(sx, sy, dz) for sx, sy in MOVES for dz in (-1, 0, 1)]

        def press(i, carry):
            for m, (sx, sy, dz) in enumerate(steps):
                for k in range(10):
                    value = turn(rows8(low_geo, (i + 1 + sx) * 80 + 8 * k), -(sy * LOW + dz))
                    if k in (4, 5) and dz:
                        value = value + float(dz)
                    stage[m * 80 + 8 * k : m * 80 + 8 * k + 8, :] = value

            def from_stage(m, h):
                return lambda: [stage[m * 80 + 16 * k + 8 * h : m * 80 + 16 * k + 8 * h + 8, :] for k in range(5)]

            spots = [[spread(low_wall, i * 16 + 4 * k + w) for k in range(3)] for w in range(WALLS)]
            found = sum_walls(spots, [from_stage(m, h) for m in range(27) for h in range(2)])
            for w in range(WALLS):
                low_wall[pl.ds(i * 16 + 12 + w, 1), :] = found[w]
            return carry

        lax.fori_loop(0, BX + 2, press, 0)

        def push(i, carry):
            for m, (sx, sy, dz) in enumerate(steps):
                for k in range(2):
                    value = turn(rows8(low_wall, (i + 1 + sx) * 16 + 8 * k), -(sy * LOW + dz))
                    if k == 1 and dz:
                        value = jnp.where(sub < 4, value + float(dz), value)
                    stage[m * 16 + 8 * k : m * 16 + 8 * k + 8, :] = value
            for h in range(2):
                t = [rows8(low_target, i * 128 + 16 * k + 8 * h) for k in range(8)]
                t[3] = t[3] + 0.5
                sums = [zero] * 4
                for m in range(27):
                    for w in range(WALLS):
                        terms = wall_pair(t, [spread(stage, 16 * m + 4 * k + w) for k in range(4)])
                        sums = [a + b for a, b in zip(sums, terms)]
                for c in range(4):
                    put8(low_sum, i * 64 + 16 * c + 8 * h, sums[c])
            return carry

        lax.fori_loop(0, BX, push, 0)
        for i in range(BX):
            for j in range(BY):
                for k in range(8):
                    base = (i * BY + j) * 64 + 8 * k
                    add = turn(low_sum[i * 64 + 8 * k : i * 64 + 8 * k + 8, :], -(j + 2) * LOW)
                    total[base : base + 8, :] = total[base : base + 8, :] + jnp.where(lane < LOW, add, 0.0)

    def wall_column(n, carry):
        flag = jnp.where(n < 15, flags_a >> jnp.minimum(n, 15), flags_b >> jnp.maximum(n - 15, 0)) & 1

        @pl.when(flag == 1)
        def _():
            kx, ky = n // 6, n % 6
            for m, (sx, sy) in enumerate(MOVES):
                h = (kx + 1 + sx) * 8 + ky + 1 + sy
                for k in range(10):
                    value = rows8(geo, h * 80 + 8 * k)
                    for v, move in enumerate((-1, 1)):
                        moved = shifted(value, move, PAD if k < 2 else None)
                        if k in (4, 5):
                            moved = moved + float(move)
                        stage[(v * 9 + m) * 80 + 8 * k : (v * 9 + m) * 80 + 8 * k + 8, :] = moved

            def from_stage(m, v, j):
                def get():
                    if v == 0:
                        h = (kx + 1 + MOVES[m][0]) * 8 + ky + 1 + MOVES[m][1]
                        return [rows8(geo, h * 80 + 16 * k + 8 * j) for k in range(5)]
                    base = ((v - 1) * 9 + m) * 80 + 8 * j
                    return [stage[base + 16 * k : base + 16 * k + 8, :] for k in range(5)]

                return get

            spots = [[spread(walls, n * 16 + 4 * k + w) for k in range(3)] for w in range(WALLS)]
            found = sum_walls(spots, [from_stage(m, v, j) for m in range(9) for v in range(3) for j in range(2)])
            for w in range(WALLS):
                walls[pl.ds(n * 16 + 12 + w, 1), :] = found[w]
            for v, move in enumerate((0, -1, 1)):
                for k in range(2):
                    value = rows8(walls, n * 16 + 8 * k)
                    if move:
                        moved = turn(value, -move)
                        if k == 0:
                            edge = lane == (127 if move > 0 else 0)
                            value = jnp.where(edge & (sub < 4), FAR, moved)
                        else:
                            value = jnp.where(sub < 4, moved + float(move), moved)
                    stage[v * 16 + 8 * k : v * 16 + 8 * k + 8, :] = value

            def over_x(x, c):
                def over_y(y, c):
                    q = x * BY + y
                    for h in range(2):
                        t = [rows8(own, q * ROWS + PART[k] + 8 * h) for k in range(8)]
                        t[3] = t[3] + 0.5
                        sums = [zero] * 4
                        for v in range(3):
                            for w in range(WALLS):
                                terms = wall_pair(t, [spread(stage, v * 16 + 4 * k + w) for k in range(4)])
                                sums = [a + b for a, b in zip(sums, terms)]
                        for c4 in range(4):
                            base = q * 64 + 16 * c4 + 8 * h
                            put8(total, base, rows8(total, base) + sums[c4])
                    return c

                return lax.fori_loop(jnp.maximum(ky - 2, 0), jnp.minimum(ky, BY - 1) + 1, over_y, c)

            lax.fori_loop(jnp.maximum(kx - 2, 0), jnp.minimum(kx, BX - 1) + 1, over_x, 0)

        return carry

    @pl.when(flags_a + flags_b > 0)
    def _():
        lax.fori_loop(0, 30, wall_column, 0)

    most = jnp.zeros((SLOTS, 128), F32)
    for q in range(COLS):
        live = own[q * ROWS : q * ROWS + 16, :] < 0.5 * FAR
        sq = jnp.zeros((SLOTS, 128), F32)
        for c in range(3):
            value = SCALE * total[q * 64 + 16 * c : q * 64 + 16 * c + 16, :]
            if c == 2:
                value = value - GRAVITY
            value = jnp.where(live, value, 0.0)
            sq = sq + value * value
            acc_out[pl.ds(c * SLOTS * COLS + q, SLOTS, stride=COLS), :] = value
        most = jnp.maximum(most, sq)
        rate = -SCALE * total[q * 64 + 48 : q * 64 + 64, :]
        rate_out[pl.ds(q, SLOTS, stride=COLS), :] = jnp.where(live, rate, 0.0)
    top[...] = jnp.zeros(top.shape, F32) + jnp.max(most)


def scale_body(tops, acc, out):
    largest = jnp.broadcast_to(jnp.max(tops[...], axis=0), (8, 128))
    step = 0.25 * jnp.sqrt(0.5 / (jnp.sqrt(largest) + 1e-6))
    for n in range(3 * SLOTS * COLS // 8):
        out[8 * n : 8 * n + 8, :] = acc[8 * n : 8 * n + 8, :] * step


def shape(*dims):
    return jax.ShapeDtypeStruct(dims, F32)


def vmem(rows):
    return pltpu.VMEM((rows, 128), F32)


def call(body, outs, operands, scratch=(), flops=0, tables=0, name=None, space=pltpu.VMEM, room=48 << 20):
    specs = [pl.BlockSpec(memory_space=pltpu.SMEM)] * tables
    specs += [pl.BlockSpec(memory_space=space)] * (len(operands) - tables)
    return pl.pallas_call(
        body,
        out_shape=outs,
        in_specs=specs,
        out_specs=jax.tree.map(lambda _: pl.BlockSpec(memory_space=pltpu.VMEM), outs),
        scratch_shapes=list(scratch),
        cost_estimate=pl.CostEstimate(flops=flops, transcendentals=0, bytes_accessed=1000000),
        compiler_params=pltpu.CompilerParams(vmem_limit_bytes=room),
        name=name,
    )(*operands)


def tables():
    inner, outer = [], []
    for q in range(COLS):
        x, y = divmod(q, BY)
        for sx, sy in MOVES:
            nx, ny = x + sx, y + sy
            if 0 <= nx < BX and 0 <= ny < BY:
                if nx * BY + ny > q:
                    inner.append((q, nx * BY + ny))
            elif (nx, ny) in SIDES:
                outer.append((q, SIDES.index((nx, ny))))
    return np.array(inner, np.int32).T.copy(), np.array(outer, np.int32).T.copy()


def on_device(fluid_offsets, fluid_velocity, fluid_density, fluid_counts, wall_offsets, wall_counts):
    flat = lambda a: a.reshape(-1, 128)
    inner, outer = tables()
    inner_table, outer_table = jnp.asarray(inner), jnp.asarray(outer)
    counts = pltpu.VMEM((BX, BY, 128), jnp.int32)
    own, right, left, up, down = call(
        pack_body,
        (shape(COLS * ROWS, 128), shape(XMSG, 128), shape(XMSG, 128), shape(YMSG, 128), shape(YMSG, 128)),
        (flat(fluid_offsets), flat(fluid_velocity), flat(fluid_density), fluid_counts, flat(wall_offsets), wall_counts),
        (vmem(576), vmem(576), vmem(192), counts, vmem(144), counts, pltpu.SemaphoreType.DMA((6,))),
        space=pltpu.HBM, room=ROOM, name="pack",
    )

    def ring(axis, step):
        size = lax.axis_size(axis)
        return [(i, i + step) for i in range(size) if 0 <= i + step < size]

    def exchange(axis, onward, backward):
        return lax.ppermute(onward, axis, ring(axis, 1)), lax.ppermute(backward, axis, ring(axis, -1))

    down_side, up_side = exchange(YZ, up, down)
    from_left, from_right = exchange(GX, right, left)
    part = call(
        partial(own_body, inner.shape[1], True), shape(COLS * 64, 128), (inner_table, own),
        (vmem(2 * COLS * 128), vmem(COLS * 4 * SLOTS * 8), vmem(COLS * 3 * 64)),
        flops=60000000, tables=1, name="inner",
    )
    down_side, up_side, from_left, from_right, part = lax.optimization_barrier(
        (down_side, up_side, from_left, from_right, part)
    )
    halo, corner_up, corner_down = call(
        forward_body, (shape(XHALO, 128), shape(CMSG, 128), shape(CMSG, 128)),
        (own, from_left, from_right), name="forward",
    )
    down_corner, up_corner = exchange(YZ, corner_up, corner_down)
    near, part = call(
        partial(sides_body, outer.shape[1]), (shape(len(SIDES) * ROWS, 128), shape(COLS * 64, 128)),
        (outer_table, own, halo, down_side, up_side, part), (vmem(2 * len(SIDES) * 128),),
        flops=60000000, tables=1, name="sides",
    )
    part, down_corner, up_corner = lax.optimization_barrier((part, down_corner, up_corner))
    acc, rate, top = call(
        rim_body,
        (shape(3 * SLOTS * COLS, 128), shape(SLOTS * COLS, 128), shape(8, 128)),
        (own, halo, near, down_side, up_side, down_corner, up_corner, part),
        (
            vmem(4 * ROWS), vmem(2 * 4 * 128), vmem(FRAME * 80), vmem(30 * 16), vmem(30 * 8), vmem(COLS * 64),
            vmem(160), vmem(256), vmem(16), vmem(144), vmem(128), vmem(27 * 80),
            vmem(7 * 80), vmem(5 * 16), vmem(3 * 128), vmem(3 * 64),
        ),
        name="rim",
    )
    devices = lax.axis_size(GX + YZ)
    tops = lax.all_to_all(jnp.broadcast_to(top[:1][None], (devices, 1, 128)), GX + YZ, 0, 0, tiled=True)
    out = call(scale_body, shape(3 * SLOTS * COLS, 128), (tops, acc), name="scale")
    return out.reshape(fluid_offsets.shape), rate.reshape(fluid_density.shape)


def solution(mesh):
    gx, yz = GX, YZ
    split = Mesh(mesh.devices.reshape(4, 2, 2, 4, 4), GX + YZ)
    placed = (
        P(None, None, gx, yz, None),
        P(None, None, gx, yz, None),
        P(None, gx, yz, None),
        P(gx, yz, None),
        P(None, None, gx, yz, None),
        P(gx, yz, None),
    )
    return jax.shard_map(
        on_device,
        mesh=split,
        in_specs=placed,
        out_specs=(P(None, None, gx, yz, None), P(None, gx, yz, None)),
        check_vma=False,
    )
```

```python
from functools import partial

import jax
import jax.numpy as jnp
import numpy as np
from jax import lax
from jax.experimental import pallas as pl
from jax.experimental.pallas import tpu as pltpu
from jax.sharding import Mesh
from jax.sharding import PartitionSpec as P

GX = ("gx_0", "gx_1", "gx_2")
YZ = ("yz_0", "yz_1")

GRAVITY = 2.0
STIFFNESS = 100.0 / 7.0
SOFT = 0.0025
SCALE = 2.5
FAR = 1.0e6
PAD = -1.0e6
BX, BY, SLOTS, WALLS = 3, 4, 16, 4
COLS = BX * BY
ROWS = 144
WIRE = 128
NEAR = 64
WALL = 112
PART = (0, 16, 32, 48, 128, 64, 80, 96)
F32 = jnp.float32


def rows8(ref, base):
    return ref[pl.ds(pl.multiple_of(base, 8), 8), :]


def spread(ref, row):
    return ref[pl.ds(row, 8, stride=0), :]


def put8(ref, base, value):
    ref[pl.ds(pl.multiple_of(base, 8), 8), :] = value


def lanes():
    return lax.broadcasted_iota(jnp.int32, (8, 128), 1)


def shifted(value, move, fill=None):
    out = pltpu.roll(value, (-move) % 128, 1)
    if fill is None:
        return out
    return jnp.where(lanes() == (127 if move > 0 else 0), fill, out)


def slope(dx, dy, dz):
    squared = dx * dx + dy * dy + dz * dz
    distance = pl.reciprocal(lax.rsqrt(squared), approx=True)
    remain = jnp.maximum(1.0 - distance, 0.0)
    return squared, remain * remain * remain


def weight(dx, dy, dz):
    squared = dx * dx + dy * dy + dz * dz
    distance = pl.reciprocal(lax.rsqrt(squared), approx=True)
    remain = jnp.maximum(1.0 - distance, 0.0)
    twice = remain * remain
    return (twice * twice) * (4.0 * distance + 1.0)


def fluid_pair(t, s):
    dx, dy, dz = t[0] - s[0], t[1] - s[1], t[2] - s[2]
    squared, cube = slope(dx, dy, dz)
    approach = (t[5] - s[5]) * dx + (t[6] - s[6]) * dy + (t[7] - s[7]) * dz
    below = (squared + SOFT) * (t[3] + s[3])
    viscous = jnp.minimum(approach, 0.0) * pl.reciprocal(below, approx=True)
    factor = cube * ((t[4] + s[4]) - viscous)
    return factor * dx, factor * dy, factor * dz, cube * approach


def wall_pair(t, s):
    dx, dy, dz = t[0] - s[0], t[1] - s[1], t[2] - s[2]
    squared, cube = slope(dx, dy, dz)
    approach = t[5] * dx + t[6] * dy + t[7] * dz
    below = (squared + SOFT) * t[3]
    viscous = jnp.minimum(approach, 0.0) * pl.reciprocal(below, approx=True)
    factor = cube * ((t[4] + s[3]) - viscous)
    return factor * dx, factor * dy, factor * dz, cube * approach


def pressure_term(rho):
    rho2 = rho * rho
    return (STIFFNESS * ((rho2 * rho2) * (rho2 * rho) - 1.0)) / rho2


def pack_body(
    off_in, vel_in, den_in, cnt_in, woff_in, wcnt_in, own, right, left, up, down,
    off, vel, den, cnt, woff, wcnt, sems,
):
    copies = [
        pltpu.make_async_copy(src, dst, sems.at[n])
        for n, (src, dst) in enumerate(
            zip((off_in, vel_in, den_in, cnt_in, woff_in, wcnt_in), (off, vel, den, cnt, woff, wcnt))
        )
    ]
    for copy in copies:
        copy.start()
    for copy in copies:
        copy.wait()
    slot = lax.broadcasted_iota(jnp.int32, (SLOTS, 128), 0)
    wslot = lax.broadcasted_iota(jnp.int32, (WALLS, 128), 0)
    for q in range(COLS):
        x, y = divmod(q, BY)
        base = q * ROWS
        live = slot < jnp.broadcast_to(cnt[x, y : y + 1, :], (SLOTS, 128))

        def take(ref, part):
            return ref[pl.ds(part * SLOTS * COLS + q, SLOTS, stride=COLS), :]

        rho = take(den, 0)
        parts = (
            jnp.where(live, take(off, 0) + float(x), FAR),
            take(off, 1) + float(y),
            take(off, 2),
            0.5 * rho,
            pressure_term(rho),
            take(vel, 0),
            take(vel, 1),
            take(vel, 2),
        )
        for at, part in zip(PART, parts):
            own[base + at : base + at + 16, :] = part
        live = wslot < jnp.broadcast_to(wcnt[x, y : y + 1, :], (WALLS, 128))

        def wtake(part):
            return woff[pl.ds(part * WALLS * COLS + q, WALLS, stride=COLS), :]

        base += WALL
        own[base : base + 4, :] = jnp.where(live, wtake(0) + float(x), FAR)
        own[base + 4 : base + 8, :] = wtake(1) + float(y)
        own[base + 8 : base + 12, :] = wtake(2)
        own[base + 12 : base + 16, :] = jnp.where(live, 1.0, 0.0)
    for ref, first in ((right, BX - 1), (left, 0)):
        for y in range(BY):
            base = (first * BY + y) * ROWS
            ref[y * WIRE : (y + 1) * WIRE, :] = own[base : base + WIRE, :]
            base = (1 * BY + y) * ROWS
            start = BY * WIRE + y * NEAR
            ref[start : start + NEAR, :] = own[base : base + NEAR, :]
    for ref, near, next_ in ((up, BY - 1, BY - 2), (down, 0, 1)):
        for x in range(BX):
            base = (x * BY + near) * ROWS
            ref[x * WIRE : (x + 1) * WIRE, :] = own[base : base + WIRE, :]
            base = (x * BY + next_) * ROWS
            start = BX * WIRE + x * NEAR
            ref[start : start + NEAR, :] = own[base : base + NEAR, :]


XMSG = BY * (WIRE + NEAR)
YMSG = BX * (WIRE + NEAR)
CMSG = 2 * WIRE + 6 * NEAR
XHALO = 8 * ROWS + 8 * NEAR


def corner_rows(ring, fx):
    if ring == 1:
        return {-1: 0, 3: WIRE, -2: 2 * WIRE, 4: 2 * WIRE + NEAR}[fx]
    return 2 * WIRE + 2 * NEAR + {-2: 0, -1: 1, 3: 2, 4: 3}[fx] * NEAR


def x_rows(fx, y):
    if fx in (-1, 3):
        return ((0 if fx < 0 else BY) + y) * ROWS
    return 8 * ROWS + ((0 if fx < 0 else BY) + y) * NEAR


def settle(src, base, dst, to, full, axis, move):
    for h in range(2):
        rho = src[base + 48 + 8 * h : base + 56 + 8 * h, :]
        for k in (0, 1, 2, 3, 5, 6, 7) if full else range(4):
            row = PART[k] + 8 * h
            value = src[base + row : base + row + 8, :]
            if k == axis:
                value = value + move
            if k == 0:
                value = jnp.where(rho > 0.0, value, FAR)
            dst[to + row : to + row + 8, :] = value
        if full:
            term = pressure_term(jnp.where(rho > 0.0, 2.0 * rho, 1.0))
            dst[to + 128 + 8 * h : to + 136 + 8 * h, :] = term
    if full:
        base, to = base + WALL, to + WALL
        mask = src[base + 12 : base + 16, :]
        for k in range(3):
            value = src[base + 4 * k : base + 4 * k + 4, :]
            if k == axis:
                value = value + move
            if k == 0:
                value = jnp.where(mask > 0.0, value, FAR)
            dst[to + 4 * k : to + 4 * k + 4, :] = value
        dst[to + 12 : to + 16, :] = mask


def forward_body(own, from_left, from_right, halo, up, down):
    for src, fx, fx2, move in ((from_left, -1, -2, -3.0), (from_right, 3, 4, 3.0)):
        for y in range(BY):
            settle(src, y * WIRE, halo, x_rows(fx, y), True, 0, move)
            settle(src, BY * WIRE + y * NEAR, halo, x_rows(fx2, y), False, 0, move)
    for ref, near, next_ in ((up, BY - 1, BY - 2), (down, 0, 1)):
        for ring, y in ((1, near), (2, next_)):
            for fx in (-2, -1, 3, 4):
                count = WIRE if (ring == 1 and fx in (-1, 3)) else NEAR
                to = corner_rows(ring, fx)
                base = x_rows(fx, y)
                ref[to : to + count, :] = halo[base : base + count, :]


def roll_columns(src, rolled, count):
    for q in range(count):
        for v, move in enumerate((-1, 1)):
            for k in range(8):
                for h in range(2):
                    base = q * ROWS + PART[k] + 8 * h
                    value = shifted(src[base : base + 8, :], move, PAD if k == 0 else None)
                    if k == 2:
                        value = value + float(move)
                    to = (v * count + q) * 128 + 16 * k + 8 * h
                    rolled[to : to + 8, :] = value


def own_body(count, selfs, tab, own, out, rolled, acc, racc):
    zero = jnp.zeros((8, 128), F32)

    def clear(i, c):
        base = i * 128
        for k in range(16):
            put8(acc, base + 8 * k, zero)
        return c

    lax.fori_loop(0, COLS * 4 * SLOTS * 8 // 128, clear, 0)

    def clear_r(i, c):
        for k in range(24):
            put8(racc, i * 192 + 8 * k, zero)
        return c

    lax.fori_loop(0, COLS, clear_r, 0)

    roll_columns(own, rolled, COLS)

    def block(t, s, v, symmetric):
        if v == 0:
            src = [[rows8(own, s * ROWS + PART[k] + 8 * h) for k in range(8)] for h in range(2)]
        else:
            base = ((v - 1) * COLS + s) * 128
            src = [[rows8(rolled, base + 16 * k + 8 * h) for k in range(8)] for h in range(2)]
        back = [[zero] * 4 for _ in range(2)]
        for i in range(SLOTS):
            dst = [spread(own, t * ROWS + PART[k] + i) for k in range(8)]
            both = [fluid_pair(dst, src[h]) for h in range(2)]
            for c in range(4):
                base = ((t * 4 + c) * SLOTS + i) * 8
                put8(acc, base, rows8(acc, base) + (both[0][c] + both[1][c]))
            if symmetric:
                for h in range(2):
                    for c in range(3):
                        back[h][c] = back[h][c] - both[h][c]
                    back[h][3] = back[h][3] + both[h][3]
        if symmetric:
            for h in range(2):
                for c in range(4):
                    base = (s * 3 + v) * 64 + 16 * c + 8 * h
                    put8(racc, base, rows8(racc, base) + back[h][c])

    def pair(e, c):
        t, s = tab[0, e], tab[1, e]
        for v in range(3):
            block(t, s, v, True)
        return c

    lax.fori_loop(0, count, pair, 0)
    if selfs:

        def alone(q, c):
            block(q, q, 0, False)
            block(q, q, 2, True)
            return c

        lax.fori_loop(0, COLS, alone, 0)

    sub = lax.broadcasted_iota(jnp.int32, (8, 128), 0)

    def gather_rows(values):
        for bit in (1, 2, 4):
            odd = (sub & bit) != 0
            values = [
                jnp.where(odd, b, a) + pltpu.roll(jnp.where(odd, a, b), bit, 0) if bit == 4
                else jnp.where(odd, b + pltpu.roll(b, bit, 0), a + pltpu.roll(a, 8 - bit, 0))
                for a, b in zip(values[0::2], values[1::2])
            ]
        return values[0]

    def finish(group, c):
        for n in range(3):
            q = group * 3 + n
            for k in range(8):
                start = (q * 4 * SLOTS + 8 * k) * 8
                value = gather_rows([rows8(acc, start + 8 * i) for i in range(8)])
                value = value + rows8(racc, q * 192 + 8 * k)
                value = value + pltpu.roll(rows8(racc, q * 192 + 64 + 8 * k), 127, 1)
                value = value + pltpu.roll(rows8(racc, q * 192 + 128 + 8 * k), 1, 1)
                put8(out, q * 64 + 8 * k, value)
        return c

    lax.fori_loop(0, COLS // 3, finish, 0)


SIDES = (
    [(-1, y) for y in range(BY)]
    + [(BX, y) for y in range(BY)]
    + [(x, -1) for x in range(BX)]
    + [(x, BY) for x in range(BX)]
)
CORNERS = [(-1, -1), (BX, -1), (-1, BY), (BX, BY)]
FRAME = (BX + 4) * (BY + 4)
LOW = 16
ROOM = 64500000
MOVES = [(sx, sy) for sx in (-1, 0, 1) for sy in (-1, 0, 1)]


def frame(fx, fy):
    return (fx + 2) * 8 + fy + 2


def turn(value, shift):
    return pltpu.roll(value, shift % 128, 1) if shift % 128 else value


def against(own, q, sources, total, halves=2, slots=SLOTS):
    t = [[rows8(own, q * ROWS + PART[k] + 8 * h) for k in range(8)] for h in range(halves)]
    sums = [[jnp.zeros((8, 128), F32)] * 4 for _ in range(halves)]
    for ref, base, at in sources:
        for j in range(slots):
            s = [spread(ref, base + at[k] + j) for k in range(8)]
            for h in range(halves):
                sums[h] = [a + b for a, b in zip(sums[h], fluid_pair(t[h], s))]
    for h in range(halves):
        for c in range(4):
            base = q * 64 + 16 * c + 8 * h
            put8(total, base, rows8(total, base) + sums[h][c])


DENSE = tuple(16 * k for k in range(8))


def crowded(refs):
    least = jnp.full((8, 128), FAR, F32)
    for ref, base in refs:
        least = jnp.minimum(least, ref[base + 8 : base + 16, :])
    return jnp.min(least) < 0.5 * FAR


def sides_body(count, tab, own, halo, from_down, from_up, inner, near, total, rolled):
    for n, (fx, fy) in enumerate(SIDES):
        if 0 <= fy < BY:
            base = x_rows(fx, fy)
            near[n * ROWS : (n + 1) * ROWS, :] = halo[base : base + ROWS, :]
        else:
            src, move = (from_down, -4.0) if fy < 0 else (from_up, 4.0)
            settle(src, fx * WIRE, near, n * ROWS, True, 1, move)
    total[...] = inner[...]
    roll_columns(near, rolled, len(SIDES))
    many_own = crowded([(own, q * ROWS) for q in range(COLS)])
    many_near = crowded([(near, n * ROWS) for n in range(len(SIDES))])

    def pair(e, carry):
        q, n = tab[0, e], tab[1, e]
        sources = [(near, n * ROWS, PART)]
        sources += [(rolled, (v * len(SIDES) + n) * 128, DENSE) for v in range(2)]
        against(own, q, sources, total)
        return carry

    def sparse_pair(e, carry):
        q, n = tab[0, e], tab[1, e]
        sources = [(near, n * ROWS, PART)]
        sources += [(rolled, (v * len(SIDES) + n) * 128, DENSE) for v in range(2)]
        against(own, q, sources, total, 1, 8)
        return carry

    few = jnp.logical_not(many_own | many_near)

    @pl.when(few)
    def _():
        lax.fori_loop(0, count, sparse_pair, 0)

    @pl.when(jnp.logical_not(few))
    def _():
        lax.fori_loop(0, count, pair, 0)


def sum_walls(spots, sources):
    zero = jnp.zeros((8, 128), F32)
    mass, load = [zero] * WALLS, [zero] * WALLS
    for get in sources:
        s = get()
        for w in range(WALLS):
            dz = spots[w][2] - s[2]
            value = weight(spots[w][0] - s[0], spots[w][1] - s[1], dz)
            mass[w] = mass[w] + value
            load[w] = load[w] + value * (s[4] - s[3] * dz)
    return [
        jnp.sum(load[w], axis=0, keepdims=True) / jnp.maximum(jnp.sum(mass[w], axis=0, keepdims=True), 1.0)
        for w in range(WALLS)
    ]


def rim_body(
    own, halo, near, down_side, up_side, down_corner, up_corner, part, acc_out, rate_out, top,
    corner, rolled, geo, walls, low_walls, total, bottom, target, wbot, wroll, rbot, stage,
    low_geo, low_wall, low_target, low_sum,
):
    zero = jnp.zeros((8, 128), F32)
    lane = lanes()
    sub = lax.broadcasted_iota(jnp.int32, (8, 128), 0)
    for n, (fx, fy) in enumerate(CORNERS):
        src, move = (down_corner, -4.0) if fy < 0 else (up_corner, 4.0)
        settle(src, corner_rows(1, fx), corner, n * ROWS, True, 1, move)
    total[...] = part[...]
    roll_columns(corner, rolled, len(CORNERS))
    for n, (fx, fy) in enumerate(CORNERS):
        q = min(max(fx, 0), BX - 1) * BY + min(max(fy, 0), BY - 1)
        sources = [(corner, n * ROWS, PART)]
        sources += [(rolled, (v * len(CORNERS) + n) * 128, DENSE) for v in range(2)]
        against(own, q, sources, total)

    def place(fx, fy):
        if 0 <= fx < BX and 0 <= fy < BY:
            return own, (fx * BY + fy) * ROWS
        if (fx, fy) in SIDES:
            return near, SIDES.index((fx, fy)) * ROWS
        return corner, CORNERS.index((fx, fy)) * ROWS

    for fx in range(-2, BX + 2):
        for fy in range(-2, BY + 2):
            to = frame(fx, fy) * 80
            if -1 <= fx <= BX and -1 <= fy <= BY:
                ref, base = place(fx, fy)
            elif 0 <= fy < BY:
                ref, base = halo, x_rows(fx, fy)
            else:
                ring = 2 if fy in (-2, BY + 1) else 1
                move = -4.0 if fy < 0 else 4.0
                if 0 <= fx < BX:
                    src, base = (down_side if fy < 0 else up_side), BX * WIRE + fx * NEAR
                else:
                    src, base = (down_corner if fy < 0 else up_corner), corner_rows(ring, fx)
                settle(src, base, geo, to, False, 1, move)
                ref, base = geo, to
            for h in range(2):
                rho = 2.0 * ref[base + 48 + 8 * h : base + 56 + 8 * h, :]
                if ref is not geo:
                    for k in range(3):
                        row = 16 * k + 8 * h
                        geo[to + row : to + row + 8, :] = ref[base + row : base + row + 8, :]
                rho2 = rho * rho
                geo[to + 48 + 8 * h : to + 56 + 8 * h, :] = GRAVITY * rho
                geo[to + 64 + 8 * h : to + 72 + 8 * h, :] = STIFFNESS * ((rho2 * rho2) * (rho2 * rho) - 1.0)

    for k in range(10):
        low, high = zero, zero
        for h in range(FRAME):
            value = geo[h * 80 + 8 * k : h * 80 + 8 * k + 8, :]
            low = jnp.where(lane == h, turn(value, h), low)
            high = jnp.where(lane == h, turn(value, h - 1), high)
        bottom[8 * k : 8 * k + 8, :] = low
        bottom[80 + 8 * k : 88 + 8 * k, :] = high + 1.0 if k in (4, 5) else high
    for k in range(16):
        low, high = zero, zero
        for q in range(COLS):
            h = frame(*divmod(q, BY))
            base = q * ROWS + PART[k // 2] + 8 * (k % 2)
            value = own[base : base + 8, :]
            low = jnp.where(lane == h, turn(value, h), low)
            high = jnp.where(lane == h, turn(value, h - 1), high)
        target[8 * k : 8 * k + 8, :] = low
        target[128 + 8 * k : 136 + 8 * k, :] = high + 1.0 if k in (4, 5) else high
    codes = [zero] * 4
    wa, wb = zero, zero
    for n in range(30):
        fx, fy = n // 6 - 1, n % 6 - 1
        ref, base = place(fx, fy)
        base += WALL
        xy, zm = ref[base : base + 8, :], ref[base + 8 : base + 16, :]
        h = frame(fx, fy)
        wa = jnp.where(lane == h, turn(xy, h), wa)
        wb = jnp.where(lane == h, turn(zm, h), wb)
        mask = jnp.max(jnp.where(sub >= 4, zm, 0.0), axis=0, keepdims=True)
        one = lane[0:1]
        high = jnp.max(jnp.where(one >= LOW - 1, mask, 0.0), axis=1, keepdims=True)
        some = jnp.max(jnp.where((one >= 1) & (one < LOW - 1), mask, 0.0), axis=1, keepdims=True)
        some = jnp.where(high > 0.0, 0.0, some)
        bit = float(1 << (n % 15))
        g = 0 if n < 15 else 1
        codes[g] = codes[g] + jnp.where(high > 0.0, bit, 0.0)
        codes[2] = jnp.maximum(codes[2], some)
        walls[n * 16 : n * 16 + 8, :] = jnp.where((lane == 0) & (sub < 4), FAR, xy)
        walls[n * 16 + 8 : n * 16 + 16, :] = zm
        keep = jnp.broadcast_to(some > 0.0, (8, 128)) & (lane >= 1) & (lane < LOW - 1)
        low_walls[n * 8 : n * 8 + 8, :] = jnp.where((sub >= 4) | keep, xy, FAR)
    wbot[0:8, :] = wa
    wbot[8:16, :] = wb
    flags_a = jnp.max(codes[0]).astype(jnp.int32)
    flags_b = jnp.max(codes[1]).astype(jnp.int32)
    low_any = jnp.max(codes[2]) > 0.0

    def from_bottom(z, h, back):
        def get():
            base = 80 * z + 8 * h
            return [turn(bottom[base + 16 * k : base + 16 * k + 8, :], back) for k in range(5)]

        return get

    spots = [[spread(wbot, 4 * k + w) for k in range(3)] for w in range(WALLS)]
    found = sum_walls(spots, [from_bottom(z, h, -(sx * 8 + sy)) for sx, sy in MOVES for z in range(2) for h in range(2)])
    for w in range(WALLS):
        wbot[12 + w : 13 + w, :] = found[w]
    for m, (sx, sy) in enumerate(MOVES):
        for k in range(2):
            wroll[16 * m + 8 * k : 16 * m + 8 * k + 8, :] = turn(wbot[8 * k : 8 * k + 8, :], -(sx * 8 + sy))
    for z in range(2):
        for h in range(2):
            t = [target[128 * z + 16 * k + 8 * h : 128 * z + 16 * k + 8 * h + 8, :] for k in range(8)]
            t[3] = t[3] + 0.5
            sums = [zero] * 4
            for m in range(9):
                for w in range(WALLS):
                    terms = wall_pair(t, [spread(wroll, 16 * m + 4 * k + w) for k in range(4)])
                    sums = [a + b for a, b in zip(sums, terms)]
            for c in range(4):
                rbot[64 * z + 16 * c + 8 * h : 64 * z + 16 * c + 8 * h + 8, :] = sums[c]
    for q in range(COLS):
        h = frame(*divmod(q, BY))
        for k in range(8):
            base = q * 64 + 8 * k
            low = turn(rbot[8 * k : 8 * k + 8, :], -h)
            high = turn(rbot[64 + 8 * k : 72 + 8 * k, :], 1 - h)
            add = jnp.where(lane == 0, low, jnp.where(lane == 1, high, 0.0))
            total[base : base + 8, :] = total[base : base + 8, :] + add

    @pl.when(low_any)
    def _():
        block = lane // LOW
        for i in range(BX + 4):
            for k in range(10):
                value = zero
                for j in range(8):
                    base = (i * 8 + j) * 80 + 8 * k
                    value = jnp.where(block == j, turn(geo[base : base + 8, :], j * LOW), value)
                low_geo[i * 80 + 8 * k : i * 80 + 8 * k + 8, :] = value
        for i in range(BX + 2):
            xy, zm = jnp.where(sub < 4, FAR, zero), zero
            for j in range(6):
                n = i * 6 + j
                xy = jnp.where(block == j + 1, turn(low_walls[n * 8 : n * 8 + 8, :], (j + 1) * LOW), xy)
                zm = jnp.where(block == j + 1, turn(walls[n * 16 + 8 : n * 16 + 16, :], (j + 1) * LOW), zm)
            low_wall[i * 16 : i * 16 + 8, :] = xy
            low_wall[i * 16 + 8 : i * 16 + 16, :] = zm
        for i in range(BX):
            for k in range(16):
                value = zero
                for j in range(BY):
                    base = (i * BY + j) * ROWS + PART[k // 2] + 8 * (k % 2)
                    value = jnp.where(block == j + 2, turn(own[base : base + 8, :], (j + 2) * LOW), value)
                low_target[i * 128 + 8 * k : i * 128 + 8 * k + 8, :] = value
        steps = [(sx, sy, dz) for sx, sy in MOVES for dz in (-1, 0, 1)]

        def press(i, carry):
            for m, (sx, sy, dz) in enumerate(steps):
                for k in range(10):
                    value = turn(rows8(low_geo, (i + 1 + sx) * 80 + 8 * k), -(sy * LOW + dz))
                    if k in (4, 5) and dz:
                        value = value + float(dz)
                    stage[m * 80 + 8 * k : m * 80 + 8 * k + 8, :] = value

            def from_stage(m, h):
                return lambda: [stage[m * 80 + 16 * k + 8 * h : m * 80 + 16 * k + 8 * h + 8, :] for k in range(5)]

            spots = [[spread(low_wall, i * 16 + 4 * k + w) for k in range(3)] for w in range(WALLS)]
            found = sum_walls(spots, [from_stage(m, h) for m in range(27) for h in range(2)])
            for w in range(WALLS):
                low_wall[pl.ds(i * 16 + 12 + w, 1), :] = found[w]
            return carry

        lax.fori_loop(0, BX + 2, press, 0)

        def push(i, carry):
            for m, (sx, sy, dz) in enumerate(steps):
                for k in range(2):
                    value = turn(rows8(low_wall, (i + 1 + sx) * 16 + 8 * k), -(sy * LOW + dz))
                    if k == 1 and dz:
                        value = jnp.where(sub < 4, value + float(dz), value)
                    stage[m * 16 + 8 * k : m * 16 + 8 * k + 8, :] = value
            for h in range(2):
                t = [rows8(low_target, i * 128 + 16 * k + 8 * h) for k in range(8)]
                t[3] = t[3] + 0.5
                sums = [zero] * 4
                for m in range(27):
                    for w in range(WALLS):
                        terms = wall_pair(t, [spread(stage, 16 * m + 4 * k + w) for k in range(4)])
                        sums = [a + b for a, b in zip(sums, terms)]
                for c in range(4):
                    put8(low_sum, i * 64 + 16 * c + 8 * h, sums[c])
            return carry

        lax.fori_loop(0, BX, push, 0)
        for i in range(BX):
            for j in range(BY):
                for k in range(8):
                    base = (i * BY + j) * 64 + 8 * k
                    add = turn(low_sum[i * 64 + 8 * k : i * 64 + 8 * k + 8, :], -(j + 2) * LOW)
                    total[base : base + 8, :] = total[base : base + 8, :] + jnp.where(lane < LOW, add, 0.0)

    def wall_column(n, carry):
        flag = jnp.where(n < 15, flags_a >> jnp.minimum(n, 15), flags_b >> jnp.maximum(n - 15, 0)) & 1

        @pl.when(flag == 1)
        def _():
            kx, ky = n // 6, n % 6
            for m, (sx, sy) in enumerate(MOVES):
                h = (kx + 1 + sx) * 8 + ky + 1 + sy
                for k in range(10):
                    value = rows8(geo, h * 80 + 8 * k)
                    for v, move in enumerate((-1, 1)):
                        moved = shifted(value, move, PAD if k < 2 else None)
                        if k in (4, 5):
                            moved = moved + float(move)
                        stage[(v * 9 + m) * 80 + 8 * k : (v * 9 + m) * 80 + 8 * k + 8, :] = moved

            def from_stage(m, v, j):
                def get():
                    if v == 0:
                        h = (kx + 1 + MOVES[m][0]) * 8 + ky + 1 + MOVES[m][1]
                        return [rows8(geo, h * 80 + 16 * k + 8 * j) for k in range(5)]
                    base = ((v - 1) * 9 + m) * 80 + 8 * j
                    return [stage[base + 16 * k : base + 16 * k + 8, :] for k in range(5)]

                return get

            spots = [[spread(walls, n * 16 + 4 * k + w) for k in range(3)] for w in range(WALLS)]
            found = sum_walls(spots, [from_stage(m, v, j) for m in range(9) for v in range(3) for j in range(2)])
            for w in range(WALLS):
                walls[pl.ds(n * 16 + 12 + w, 1), :] = found[w]
            for v, move in enumerate((0, -1, 1)):
                for k in range(2):
                    value = rows8(walls, n * 16 + 8 * k)
                    if move:
                        moved = turn(value, -move)
                        if k == 0:
                            edge = lane == (127 if move > 0 else 0)
                            value = jnp.where(edge & (sub < 4), FAR, moved)
                        else:
                            value = jnp.where(sub < 4, moved + float(move), moved)
                    stage[v * 16 + 8 * k : v * 16 + 8 * k + 8, :] = value

            def over_x(x, c):
                def over_y(y, c):
                    q = x * BY + y
                    for h in range(2):
                        t = [rows8(own, q * ROWS + PART[k] + 8 * h) for k in range(8)]
                        t[3] = t[3] + 0.5
                        sums = [zero] * 4
                        for v in range(3):
                            for w in range(WALLS):
                                terms = wall_pair(t, [spread(stage, v * 16 + 4 * k + w) for k in range(4)])
                                sums = [a + b for a, b in zip(sums, terms)]
                        for c4 in range(4):
                            base = q * 64 + 16 * c4 + 8 * h
                            put8(total, base, rows8(total, base) + sums[c4])
                    return c

                return lax.fori_loop(jnp.maximum(ky - 2, 0), jnp.minimum(ky, BY - 1) + 1, over_y, c)

            lax.fori_loop(jnp.maximum(kx - 2, 0), jnp.minimum(kx, BX - 1) + 1, over_x, 0)

        return carry

    @pl.when(flags_a + flags_b > 0)
    def _():
        lax.fori_loop(0, 30, wall_column, 0)

    most = jnp.zeros((SLOTS, 128), F32)
    for q in range(COLS):
        live = own[q * ROWS : q * ROWS + 16, :] < 0.5 * FAR
        sq = jnp.zeros((SLOTS, 128), F32)
        for c in range(3):
            value = SCALE * total[q * 64 + 16 * c : q * 64 + 16 * c + 16, :]
            if c == 2:
                value = value - GRAVITY
            value = jnp.where(live, value, 0.0)
            sq = sq + value * value
            acc_out[pl.ds(c * SLOTS * COLS + q, SLOTS, stride=COLS), :] = value
        most = jnp.maximum(most, sq)
        rate = -SCALE * total[q * 64 + 48 : q * 64 + 64, :]
        rate_out[pl.ds(q, SLOTS, stride=COLS), :] = jnp.where(live, rate, 0.0)
    top[...] = jnp.zeros(top.shape, F32) + jnp.max(most)


def scale_body(tops, acc, out):
    largest = jnp.broadcast_to(jnp.max(tops[...], axis=0), (8, 128))
    step = 0.25 * jnp.sqrt(0.5 / (jnp.sqrt(largest) + 1e-6))
    for n in range(3 * SLOTS * COLS // 8):
        out[8 * n : 8 * n + 8, :] = acc[8 * n : 8 * n + 8, :] * step


def shape(*dims):
    return jax.ShapeDtypeStruct(dims, F32)


def vmem(rows):
    return pltpu.VMEM((rows, 128), F32)


def call(body, outs, operands, scratch=(), flops=0, tables=0, name=None, space=pltpu.VMEM, room=48 << 20):
    specs = [pl.BlockSpec(memory_space=pltpu.SMEM)] * tables
    specs += [pl.BlockSpec(memory_space=space)] * (len(operands) - tables)
    return pl.pallas_call(
        body,
        out_shape=outs,
        in_specs=specs,
        out_specs=jax.tree.map(lambda _: pl.BlockSpec(memory_space=pltpu.VMEM), outs),
        scratch_shapes=list(scratch),
        cost_estimate=pl.CostEstimate(flops=flops, transcendentals=0, bytes_accessed=1000000),
        compiler_params=pltpu.CompilerParams(vmem_limit_bytes=room),
        name=name,
    )(*operands)


def tables():
    inner, outer = [], []
    for q in range(COLS):
        x, y = divmod(q, BY)
        for sx, sy in MOVES:
            nx, ny = x + sx, y + sy
            if 0 <= nx < BX and 0 <= ny < BY:
                if nx * BY + ny > q:
                    inner.append((q, nx * BY + ny))
            elif (nx, ny) in SIDES:
                outer.append((q, SIDES.index((nx, ny))))
    return np.array(inner, np.int32).T.copy(), np.array(outer, np.int32).T.copy()


def on_device(fluid_offsets, fluid_velocity, fluid_density, fluid_counts, wall_offsets, wall_counts):
    flat = lambda a: a.reshape(-1, 128)
    inner, outer = tables()
    inner_table, outer_table = jnp.asarray(inner), jnp.asarray(outer)
    counts = pltpu.VMEM((BX, BY, 128), jnp.int32)
    own, right, left, up, down = call(
        pack_body,
        (shape(COLS * ROWS, 128), shape(XMSG, 128), shape(XMSG, 128), shape(YMSG, 128), shape(YMSG, 128)),
        (flat(fluid_offsets), flat(fluid_velocity), flat(fluid_density), fluid_counts, flat(wall_offsets), wall_counts),
        (vmem(576), vmem(576), vmem(192), counts, vmem(144), counts, pltpu.SemaphoreType.DMA((6,))),
        space=pltpu.HBM, room=ROOM, name="pack",
    )

    def ring(axis, step):
        size = lax.axis_size(axis)
        return [(i, i + step) for i in range(size) if 0 <= i + step < size]

    def exchange(axis, onward, backward):
        return lax.ppermute(onward, axis, ring(axis, 1)), lax.ppermute(backward, axis, ring(axis, -1))

    down_side, up_side = exchange(YZ, up, down)
    from_left, from_right = exchange(GX, right, left)
    part = call(
        partial(own_body, inner.shape[1], True), shape(COLS * 64, 128), (inner_table, own),
        (vmem(2 * COLS * 128), vmem(COLS * 4 * SLOTS * 8), vmem(COLS * 3 * 64)),
        flops=60000000, tables=1, name="inner",
    )
    down_side, up_side, from_left, from_right, part = lax.optimization_barrier(
        (down_side, up_side, from_left, from_right, part)
    )
    halo, corner_up, corner_down = call(
        forward_body, (shape(XHALO, 128), shape(CMSG, 128), shape(CMSG, 128)),
        (own, from_left, from_right), name="forward",
    )
    down_corner, up_corner = exchange(YZ, corner_up, corner_down)
    near, part = call(
        partial(sides_body, outer.shape[1]), (shape(len(SIDES) * ROWS, 128), shape(COLS * 64, 128)),
        (outer_table, own, halo, down_side, up_side, part), (vmem(2 * len(SIDES) * 128),),
        flops=60000000, tables=1, name="sides",
    )
    part, down_corner, up_corner = lax.optimization_barrier((part, down_corner, up_corner))
    acc, rate, top = call(
        rim_body,
        (shape(3 * SLOTS * COLS, 128), shape(SLOTS * COLS, 128), shape(8, 128)),
        (own, halo, near, down_side, up_side, down_corner, up_corner, part),
        (
            vmem(4 * ROWS), vmem(2 * 4 * 128), vmem(FRAME * 80), vmem(30 * 16), vmem(30 * 8), vmem(COLS * 64),
            vmem(160), vmem(256), vmem(16), vmem(144), vmem(128), vmem(27 * 80),
            vmem(7 * 80), vmem(5 * 16), vmem(3 * 128), vmem(3 * 64),
        ),
        name="rim",
    )
    devices = lax.axis_size(GX + YZ)
    tops = lax.all_to_all(jnp.broadcast_to(top[:1][None], (devices, 1, 128)), GX + YZ, 0, 0, tiled=True)
    out = call(scale_body, shape(3 * SLOTS * COLS, 128), (tops, acc), name="scale")
    return out.reshape(fluid_offsets.shape), rate.reshape(fluid_density.shape)


def solution(mesh):
    gx, yz = GX, YZ
    split = Mesh(mesh.devices.reshape(4, 2, 2, 4, 4), GX + YZ)
    placed = (
        P(None, None, gx, yz, None),
        P(None, None, gx, yz, None),
        P(None, gx, yz, None),
        P(gx, yz, None),
        P(None, None, gx, yz, None),
        P(gx, yz, None),
    )
    return jax.shard_map(
        on_device,
        mesh=split,
        in_specs=placed,
        out_specs=(P(None, None, gx, yz, None), P(None, gx, yz, None)),
        check_vma=False,
    )
```
